32 devices in a mesh: lon: 8 (over z, x), lat: 4 (over y, core).
Axes of the slice: x: 2, y: 2, z: 4, core: 2. Of those that a mesh axis runs over, the one named last changes fastest.
Arguments:
- state: float32 [8, 64, 16, 1024], P(None, None, 'lat', 'lon'), may hold values from -6 to 6
- winds: float32 [2, 64, 16, 1024], P(None, None, 'lat', 'lon'), may hold values from -0.3 to 0.3
- diffusivity: float32 [16, 1024], P('lat', 'lon'), may hold values from 0.05 to 0.2
- sounding_cell: int32 [2, 4096], P(None, ('lon', 'lat')), may hold values from 0 to 511
- sounding_owner: int32 [2, 4096, 1], P(None, ('lon', 'lat')), may hold values from 0 to 31; in each aligned block of 128 rows (0 to 127, 128 to 255, ..., all dimensions but the last counted through in order) at most 6 rows name the same one
- step_counts: int32 [2], replicated, may hold values from 1 to 4
- channel_list: int32 [512], replicated, may hold values from 0 to 615
- absorb_table: float32 [512, 616], replicated, may hold values from -0.25 to 0.25
- emit_table: float32 [512, 616], replicated, may hold values from -0.25 to 0.25
- obs_weight: float32 [616], replicated, may hold values from 0.5 to 4
- observed: float32 [2, 32, 32, 6, 512], P(None, ('lon', 'lat')), may hold values from -6 to 6
Outputs:
- gradient: float32 [8, 64, 16, 1024], P(None, None, 'lat', 'lon')
The draws below stay inside these ranges and needn't reach their ends.
Inputs may be any that keep to these rules, and one draw needn't show every extreme that they name: `sounding_owner`: in one slot, at most 6 soundings of one tile's list name the same owner. `sounding_cell`: columns are numbered row by row within the tile. `channel_list`: entries may repeat.
All inputs are finite; a program needn't handle non-finite values.
Results may differ from the reference program's by a relative error of at most 0.00022.
Values sent between devices are 32-bit elements; how exact they have to be, the bound alone decides.
A program may use at most 128 MiB of HBM per device.

```python
import math
from functools import partial
import jax
import jax.numpy as jnp
import numpy as np
from jax import lax

VARS = 8
LEV = 64
CHAN = 616
USED = 512
CLAT = 4
CLON = 128
SND = 128
MAXSTEP = 4
SLOTS = 2
PROF = 512
NLAT = 16
NLON = 1024
SOUNDINGS = 4096
CAP = 6
N_LAT = 4
DEVICES = 32


def plant(drawn, rng, smallest, top_value):
    longest = drawn.shape.index(max(drawn.shape))
    spots = []
    for shift in (0, 1):
        where = [jax.random.randint(jax.random.fold_in(rng, axis), (), 0, length) for axis, length in enumerate(drawn.shape)]
        where[longest] = (where[longest] + shift) % drawn.shape[longest]
        spots.append(tuple(where))
    return drawn.at[spots[0]].set(smallest).at[spots[1]].set(top_value)


def level_of(rng, dims, cuts, least, largest):
    def one(position, blocks):
        steps = jax.random.uniform(jax.random.fold_in(jax.random.fold_in(rng, 6), position), (blocks,), jnp.float32, least / len(cuts), largest / len(cuts))
        return jnp.repeat(jnp.exp(steps), dims[position] // blocks).reshape((-1,) + (1,) * (len(dims) - position - 1))

    level = one(*cuts[0])
    for cut in cuts[1:]:
        level = level * one(*cut)
    return level


def assign_block(rng, own, number, rows, count, top, most, slope):
    order = jax.random.permutation(rng, count)
    packed, ordinary = load_shares(count, rows * top, most, slope, True), load_shares(count, rows * top, most, slope, False)
    places = jnp.arange(count)

    def named(sizes, offset_by):
        used = int((sizes > 0).sum())
        fixed = max(1, used // 4)
        shifted = fixed + (places - fixed + offset_by * (used - fixed)) % max(1, count - fixed)
        return jnp.zeros((count,), jnp.int32).at[order[jnp.where(places < fixed, places, shifted)]].set(jnp.asarray(sizes, jnp.int32))

    sizes = jnp.where(number % 4 == 0, named(packed, number // 4), named(ordinary, number - number // 4 - 1))
    mixed = jax.random.permutation(jax.random.fold_in(own, 3), count)
    source_of, taker = mixed[0:count // 2 * 2:2], mixed[1:count // 2 * 2:2]
    margin = jnp.minimum(sizes[source_of] - 1, most - sizes[taker]) // 2
    margin = jnp.where((source_of == order[0]) | (taker == order[0]) | (sizes[taker] == 0), 0, jnp.maximum(margin, 0))
    shifted = jax.random.randint(jax.random.fold_in(own, 4), (count // 2,), 0, 1 << 20) % (margin + 1)
    sizes = sizes.at[source_of].add(-shifted).at[taker].add(shifted)
    labels = jnp.searchsorted(jnp.cumsum(sizes), jnp.arange(rows * top), side="right").astype(jnp.int32)
    grid = labels.reshape(top, rows).T
    grid = grid[jax.random.permutation(jax.random.fold_in(own, 1), rows)]
    offset_by = jax.random.randint(jax.random.fold_in(own, 2), (rows, 1), 0, top)
    return jnp.take_along_axis(grid, (jnp.arange(top)[None, :] + offset_by) % top, axis=1)


def load_shares(count, total, most, skew, full):
    loads = [(1 << 20) // math.isqrt(grade ** skew) + 1 for grade in range(1, count + 1)]
    largest = most if full else min(most, max(-(-total // count), total * loads[0] // sum(loads)))
    least = 1 if total - largest >= count - 1 else 0
    counts, surplus = [largest] + [least] * (count - 1), total - largest - least * (count - 1)
    while surplus > 0:
        movable = [i for i in range(1, count) if counts[i] < largest] or [i for i in range(1, count) if counts[i] < most]
        mass, budget = sum([loads[i] for i in movable]), surplus
        for i in movable:
            extra = min(most - counts[i], max(1, budget * loads[i] // mass), surplus)
            counts[i] = counts[i] + extra
            surplus = surplus - extra
    return np.array(counts)


def centred(own_key, extent, deviation, reach, split=(), kind=jnp.bfloat16):
    values = jax.random.normal(own_key, extent, jnp.float32) * deviation
    if len(split) > 0:
        values = level_of(own_key, extent, split, -0.22, 0.18) * values
    return jnp.clip(values, min=-reach, max=reach).astype(kind)


def setup_inputs(seed: int = 0) -> dict:
    key_list = jax.random.split(jax.random.key(seed), 12)
    state = centred(key_list[0], (VARS, LEV, NLAT, NLON), 1.0, 6.0, ((2, 4), (3, 8)), jnp.float32)
    winds = jnp.clip(jax.random.uniform(key_list[1], (2, LEV, NLAT, NLON), jnp.float32, -0.3, 0.3) * level_of(key_list[1], (2, LEV, NLAT, NLON), ((2, 4), (3, 8)), -0.4, 0.0), -0.3, 0.3)
    diffusivity = jnp.clip(0.05 + 0.15 * jax.random.uniform(key_list[2], (NLAT, NLON), jnp.float32) ** level_of(key_list[2], (NLAT, NLON), ((0, 4), (1, 8)), -0.2, 0.2), 0.05, 0.2)
    sounding_cell = plant(jax.random.randint(key_list[3], (SLOTS, SOUNDINGS), 0, CLAT * CLON), jax.random.fold_in(key_list[3], 1), 0, (CLAT * CLON) - 1).astype(jnp.int32)
    sounding_owner_keys = jax.random.split(jax.random.fold_in(key_list[4], 1), SLOTS * SOUNDINGS // SND)
    sounding_owner_turns = jax.random.permutation(jax.random.fold_in(key_list[4], 3), SLOTS * SOUNDINGS // SND)
    sounding_owner = jax.vmap(lambda own, number: assign_block(jax.random.fold_in(key_list[4], 2), own, number, SND, DEVICES, 1, CAP, 2))(sounding_owner_keys, sounding_owner_turns).reshape((SLOTS, SOUNDINGS, 1))
    step_counts = jax.random.randint(key_list[5], (SLOTS,), 1, MAXSTEP + 1).astype(jnp.int32)
    channel_list = plant(jax.random.randint(key_list[6], (USED,), 0, CHAN), jax.random.fold_in(key_list[6], 1), 0, CHAN - 1).astype(jnp.int32)
    absorb_table = centred(key_list[7], (PROF, CHAN), PROF ** -0.5, 0.25, (), jnp.float32)
    emit_table = centred(key_list[8], (PROF, CHAN), PROF ** -0.5, 0.25, (), jnp.float32)
    obs_weight = jnp.clip(jnp.exp(jax.random.uniform(key_list[9], (CHAN,), jnp.float32, math.log(0.5), math.log(4.0))), 0.5, 4.0)
    observed = centred(key_list[10], (SLOTS, DEVICES, DEVICES, CAP, USED), 1.0, 6.0, ((1, 32),), jnp.float32)
    return {"state": state, "winds": winds, "diffusivity": diffusivity, "sounding_cell": sounding_cell, "sounding_owner": sounding_owner, "step_counts": step_counts, "channel_list": channel_list, "absorb_table": absorb_table, "emit_table": emit_table, "obs_weight": obs_weight, "observed": observed}


HIGHEST_MODE = lax.Precision.HIGHEST

def pad_field(values):
    wrapped = jnp.concatenate([values[..., -1:], values, values[..., :1]], axis=-1)
    widths = [(0, 0)] * (values.ndim - 2) + [(1, 1), (0, 0)]
    return jnp.pad(wrapped, widths)

def make_coef(winds, diffusivity):
    return jnp.stack([winds[0] * 0.5 + diffusivity, winds[0] * 0.5 - diffusivity, winds[1] * 0.5 + diffusivity, winds[1] * 0.5 - diffusivity])

def advance(padded, coef_pad):
    centre = padded[:, :, 1:-1, 1:-1]
    lon_band = padded[:, :, 1:-1, :]
    flux_lon = coef_pad[0][:, 1:-1, :-1] * lon_band[..., :-1] + coef_pad[1][:, 1:-1, :-1] * lon_band[..., 1:]
    lat_band = padded[:, :, :, 1:-1]
    flux_lat = coef_pad[2][:, :-1, 1:-1] * lat_band[:, :, :-1, :] + coef_pad[3][:, :-1, 1:-1] * lat_band[:, :, 1:, :]
    return centre - (flux_lon[..., 1:] - flux_lon[..., :-1]) - (flux_lat[:, :, 1:, :] - flux_lat[:, :, :-1, :])

def retreat(padded, coef_pad):
    centre = padded[:, :, 1:-1, 1:-1]
    lon_band = padded[:, :, 1:-1, :]
    step_lon = lon_band[..., 1:] - lon_band[..., :-1]
    result = centre + coef_pad[0][:, 1:-1, 1:-1] * step_lon[..., 1:] + coef_pad[1][:, 1:-1, :-2] * step_lon[..., :-1]
    lat_band = padded[:, :, :, 1:-1]
    step_lat = lat_band[:, :, 1:, :] - lat_band[:, :, :-1, :]
    result = result + coef_pad[2][:, 1:-1, 1:-1] * step_lat[:, :, 1:, :] + coef_pad[3][:, :-2, 1:-1] * step_lat[:, :, :-1, :]
    return result

def select_channels(channel_list, absorb_table, emit_table, obs_weight):
    picker = (jnp.arange(obs_weight.shape[0], dtype=jnp.int32)[:, None] == channel_list[None, :]).astype(jnp.float32)
    absorb = jnp.dot(absorb_table, picker, precision=HIGHEST_MODE, preferred_element_type=jnp.float32)
    emission = jnp.dot(emit_table, picker, precision=HIGHEST_MODE, preferred_element_type=jnp.float32)
    weight = jnp.dot(obs_weight[None, :], picker, precision=HIGHEST_MODE, preferred_element_type=jnp.float32)[0]
    return (absorb, emission, weight)

def radiance(profiles, absorb, emission):
    optical = jnp.dot(profiles, absorb, precision=HIGHEST_MODE, preferred_element_type=jnp.float32)
    bright = jnp.dot(profiles, emission, precision=HIGHEST_MODE, preferred_element_type=jnp.float32)
    return jnp.exp(-jax.nn.softplus(optical)) * bright

def slot_gradient(state_now, slot_index, sounding_cell, sounding_owner, observed, absorb, emission, weight):
    sounding_cells = sounding_cell[slot_index].reshape(DEVICES, SND)
    owners = sounding_owner[slot_index, :, 0].reshape(DEVICES, SND)
    owner_hit = (owners[:, :, None] == jnp.arange(DEVICES, dtype=jnp.int32)[None, None, :]).astype(jnp.int32)
    owner_rank = lax.optimization_barrier(jnp.sum(jnp.cumsum(owner_hit, axis=1) * owner_hit, axis=2)) - 1
    home_index = jnp.broadcast_to(jnp.arange(DEVICES, dtype=jnp.int32)[:, None], (DEVICES, SND))
    wanted = observed[slot_index, owners, home_index, owner_rank].reshape(DEVICES * SND, USED)
    lat_rows = (home_index % N_LAT * CLAT + sounding_cells // CLON).reshape(-1).astype(jnp.int32)
    lon_cols = (home_index // N_LAT * CLON + sounding_cells % CLON).reshape(-1).astype(jnp.int32)
    profiles = state_now[:, :, lat_rows, lon_cols].reshape(PROF, DEVICES * SND).T
    evolved, pullback = jax.vjp(partial(radiance, absorb=absorb, emission=emission), profiles)
    departure = weight[None, :] * (evolved - wanted)
    adjoint_cols = pullback(departure)[0]
    placed = adjoint_cols.T.reshape(VARS, LEV, DEVICES * SND)
    return jnp.zeros_like(state_now).at[:, :, lat_rows, lon_cols].add(placed)

def reference(state, winds, diffusivity, sounding_cell, sounding_owner, step_counts, channel_list, absorb_table, emit_table, obs_weight, observed):
    coef_pad = pad_field(make_coef(winds, diffusivity))
    absorb, emission, weight = select_channels(channel_list, absorb_table, emit_table, obs_weight)
    state_now = state
    slot_fields = []
    for slot_index in range(SLOTS):
        for step_index in range(MAXSTEP):
            state_now = jnp.where(step_index < step_counts[slot_index], advance(pad_field(state_now), coef_pad), state_now)
        slot_fields.append(state_now)
    gradients = [slot_gradient(slot_fields[slot_index], slot_index, sounding_cell, sounding_owner, observed, absorb, emission, weight) for slot_index in range(SLOTS)]
    adjoint = jnp.zeros_like(state)
    for slot_index in reversed(range(SLOTS)):
        adjoint = adjoint + gradients[slot_index]
        for step_index in range(MAXSTEP):
            adjoint = jnp.where(step_index < step_counts[slot_index], retreat(pad_field(adjoint), coef_pad), adjoint)
    return adjoint
```

```python
from functools import partial

import jax
import jax.numpy as jnp
from jax import lax
from jax.experimental import pallas as pl
from jax.experimental.pallas import tpu as pltpu
from jax.sharding import PartitionSpec as P

MAXSTEP = 4
LANES = 128
EXT = 8
PAD = 16
COLS = 24
MESH_ID = pl.DeviceIdType.MESH
FIRST = ((0,), (0,))
LAST = ((1,), (1,))


def split2(v):
    high = v.astype(jnp.bfloat16)
    return high, (v - high.astype(jnp.float32)).astype(jnp.bfloat16)


def split3(v):
    high = v.astype(jnp.bfloat16)
    rest = v - high.astype(jnp.float32)
    mid = rest.astype(jnp.bfloat16)
    return high, mid, (rest - mid.astype(jnp.float32)).astype(jnp.bfloat16)


def dot(a, b, dims=((1,), (0,))):
    return lax.dot_general(a, b, (dims, ((), ())), preferred_element_type=jnp.float32)


def one_hot(row, size):
    return (row == lax.broadcasted_iota(jnp.int32, (size, row.shape[1]), 0)).astype(
        jnp.float32).astype(jnp.bfloat16)


def whole_kernel(total, lat_count, lon_count, *refs):
    (steps_ref, state_hbm, winds_hbm, diff_hbm, obs_hbm, absorb_hbm, emit_hbm, cell_ref, owner_ref, chan_ref,
     weight_ref, out_ref,
     state, winds, diff, obs, tables, TB, AE, WS, H, Y, F, B, PK, PKU, SB, GOT,
     local_sem, pk_s, pk_r, row_s, row_r, lon_s, lon_r, diag_s, diag_r, lat_s, lat_r, obs_s, obs_r) = refs
    groups, rows = H.shape[1], H.shape[2] - 2
    width = state.shape[1]
    span = width + 2 * EXT
    levels = winds.shape[0] // (2 * rows)
    devices = lat_count * lon_count
    slots, capacity, _, used = obs.shape
    chunks = used // LANES
    block = SB.shape[1] // devices
    channels, prof = tables.shape[1:]
    cells = rows * width
    soundings = cell_ref.shape[1]
    lat = lax.axis_index("lat")
    lon = lax.axis_index("lon")
    me = lon * lat_count + lat
    east = lax.rem(lon + 1, lon_count)
    west = lax.rem(lon + lon_count - 1, lon_count)
    has_up = lat > 0
    has_down = lat < lat_count - 1
    up, down = lat - 1, lat + 1
    own = pl.ds(PAD, width)
    wide = pl.ds(PAD - EXT, span)
    head, tail = pl.ds(PAD, EXT), pl.ds(PAD + width - EXT, EXT)
    before, after = pl.ds(PAD - EXT, EXT), pl.ds(PAD + width, EXT)
    inner = pl.ds(1, rows)
    top, bottom, above, below = 1, rows, 0, rows + 1

    loads = [pltpu.make_async_copy(src, dst, local_sem.at[n]) for n, (src, dst) in enumerate((
        (state_hbm, state), (winds_hbm, winds), (diff_hbm, diff), (obs_hbm, obs),
        (absorb_hbm, tables.at[0]), (emit_hbm, tables.at[1])))]
    for load in loads:
        load.start()
    barrier = pltpu.get_barrier_semaphore()

    @pl.loop(1, devices)
    def _(j):
        other = (me + j) % devices
        pl.semaphore_signal(barrier, inc=1, device_id={"lon": other // lat_count, "lat": other % lat_count},
                            device_id_type=MESH_ID)

    def remote(src, dst, s, r, to_lat, to_lon):
        return pltpu.make_async_remote_copy(
            src, dst, s, r, device_id={"lon": to_lon, "lat": to_lat}, device_id_type=MESH_ID)

    def hand_over(k, j):
        other = (me + j) % devices
        return remote(SB.at[k, pl.ds(other * block, block)], GOT.at[k, pl.ds(me * block, block)],
                      obs_s.at[k, j], obs_r.at[k, j], other % lat_count, other // lat_count)

    def pk_lon():
        return (remote(PK.at[:, :, tail], PK.at[:, :, before], pk_s.at[0], pk_r.at[0], lat, east),
                remote(PK.at[:, :, head], PK.at[:, :, after], pk_s.at[1], pk_r.at[1], lat, west))

    def pk_down(n):
        src, dst, to_lon = ((own, own, lon), (tail, before, east), (head, after, west))[n]
        return remote(PK.at[1, rows - 1, src], PKU.at[dst], pk_s.at[2 + n], pk_r.at[2 + n], down, to_lon)

    def lon_halo(X, n, m):
        return (remote(X.at[n, :, inner, tail], X.at[n, :, inner, before], lon_s.at[m, 0], lon_r.at[m, 0], lat, east),
                remote(X.at[n, :, inner, head], X.at[n, :, inner, after], lon_s.at[m, 1], lon_r.at[m, 1], lat, west))

    def diag_up(X, m, n):
        src, dst, to_lon = ((tail, before, east), (head, after, west))[n]
        return remote(X.at[0, :, top, src], X.at[0, :, below, dst], diag_s.at[m, n], diag_r.at[m, n], up, to_lon)

    def diag_down(X, m, n):
        src, dst, to_lon = ((tail, before, east), (head, after, west))[n]
        return remote(X.at[0, :, bottom, src], X.at[0, :, above, dst], diag_s.at[m, 2 + n], diag_r.at[m, 2 + n],
                      down, to_lon)

    def row_up(X, m, g):
        return remote(X.at[0, g, top, own], X.at[0, g, below, own], row_s.at[m, g, 0], row_r.at[m, g, 0], up, lon)

    def row_down(X, m, g):
        return remote(X.at[0, g, bottom, own], X.at[0, g, above, own], row_s.at[m, g, 1], row_r.at[m, g, 1], down, lon)

    def lat_up(X, m, s, g):
        return remote(X.at[s, g, top, wide], X.at[s, g, below, wide], lat_s.at[m, s, g, 0], lat_r.at[m, s, g, 0], up, lon)

    def lat_down(X, m, s, g):
        return remote(X.at[s, g, bottom, wide], X.at[s, g, above, wide], lat_s.at[m, s, g, 1], lat_r.at[m, s, g, 1],
                      down, lon)

    def start_up_down(upward, downward):
        @pl.when(has_up)
        def _():
            for copy in upward:
                copy().start()

        @pl.when(has_down)
        def _():
            for copy in downward:
                copy().start()

    def wait_rows(upward, downward):
        @pl.when(has_down)
        def _():
            upward().wait_recv()

        @pl.when(has_up)
        def _():
            downward().wait_recv()

    loads[0].wait()

    @pl.loop(0, groups)
    def _(g):
        for r in range(rows):
            H[0, g, r + 1, own, :] = state[pl.ds(g * LANES * rows + r, LANES, stride=rows), :].T

    loads[1].wait()
    loads[2].wait()
    for i in range(2):
        for r in range(rows):
            w = winds[pl.ds(i * levels * rows + r, levels, stride=rows), :] * 0.5
            d = diff[pl.ds(r, 1), :]
            PK[i, r, own, :] = jnp.concatenate([w + d, w - d], axis=0).T

    edge = jnp.zeros((span, LANES), jnp.float32)

    @pl.when(jnp.logical_not(has_up))
    def _():
        PKU[wide, :] = edge

        @pl.loop(0, total * groups)
        def _(n):
            for X in (H, Y):
                X[n // groups, n % groups, above, wide, :] = edge

    @pl.when(jnp.logical_not(has_down))
    def _():
        @pl.loop(0, total * groups)
        def _(n):
            for X in (H, Y):
                X[n // groups, n % groups, below, wide, :] = edge

    loads[3].wait()

    @pl.loop(0, slots)
    def _(k):
        for c in range(capacity):
            for h in range(chunks):
                SB[k, pl.ds(c * chunks + h, devices, stride=block), :] = obs[k, c, :, pl.ds(h * LANES, LANES)]
        for c in range(capacity * chunks, block):
            SB[k, pl.ds(c, devices, stride=block), :] = jnp.zeros((devices, LANES), jnp.float32)
        GOT[k, pl.ds(me * block, block), :] = SB[k, pl.ds(me * block, block), :]

    pl.semaphore_wait(barrier, devices - 1)

    for copy in pk_lon():
        copy.start()
    start_up_down((), [partial(pk_down, n) for n in range(3)])
    for copy in lon_halo(H, 0, 0):
        copy.start()

    @pl.loop(0, groups)
    def _(g):
        start_up_down([lambda: row_up(H, 0, g)], [lambda: row_down(H, 0, g)])

    start_up_down([partial(diag_up, H, 0, n) for n in range(2)], [partial(diag_down, H, 0, n) for n in range(2)])

    loads[4].wait()
    loads[5].wait()
    part = channels // 7

    @pl.loop(0, 14)
    def _(n):
        at = pl.ds(n % 7 * part, part)
        high, low = split2(tables[n // 7, at, :])
        TB[n // 7, at, pl.ds(0, prof)] = high
        TB[n // 7, at, pl.ds(prof, prof)] = low

    weights = jnp.concatenate([jnp.broadcast_to(v, (8, channels)) for v in split3(weight_ref[...])], axis=0)

    @pl.loop(0, chunks)
    def _(b):
        column = jnp.broadcast_to(chan_ref[pl.ds(b, 1), :].astype(jnp.float32), (LANES, LANES)).T
        column = jnp.concatenate([column] * -(-channels // LANES), axis=1)[:, :channels]
        picker = (column == lax.broadcasted_iota(jnp.int32, (LANES, channels), 1).astype(jnp.float32)).astype(
            jnp.float32).astype(jnp.bfloat16)
        w = dot(weights, picker, LAST)
        WS[pl.ds(b, 1), :] = w[0:1] + w[8:9] + w[16:17]
        for t in range(2):
            AE[pl.ds(t * used + b * LANES, LANES), :] = dot(picker, TB[t]).astype(jnp.bfloat16)

    for copy in pk_lon():
        copy.wait_recv()

    @pl.when(has_up)
    def _():
        for n in range(3):
            pk_down(n).wait_recv()

    lower = lax.broadcasted_iota(jnp.int32, (span, LANES), 1) < levels

    def unpack(v):
        other = pltpu.roll(v, levels, 1)
        return jnp.where(lower, v, other), jnp.where(lower, other, v)

    for r in range(rows):
        a, b = unpack(PK[0, r, wide, :])
        aw, bw = unpack(PK[0, r, pl.ds(PAD - EXT - 1, span), :])
        al, bl = unpack(PK[1, r, wide, :])
        au, bu = unpack(PKU[wide, :] if r == 0 else PK[1, r - 1, wide, :])
        centre = 1.0 - a + bw - al + bu
        for n, v in enumerate((centre, -b, aw, -bl, au)):
            F[n, r] = v
        for n, v in enumerate((centre, a, -bw, al, -bu)):
            B[n, r] = v

    first_count = steps_ref[0]
    second_count = steps_ref[1]
    kept = min(MAXSTEP, total - 1)

    def advance(X, C, s, g, flag=None):
        for c in range(0, span, COLS):
            at = pl.ds(PAD - EXT + c, COLS)
            cat = pl.ds(c, COLS)
            row = [X[s, g, r, at, :] for r in range(rows + 2)]
            for r in range(rows):
                new = C[0, r, cat, :] * row[r + 1]
                new = new + C[3, r, cat, :] * row[r + 2]
                new = new + C[4, r, cat, :] * row[r]
                new = new + C[1, r, cat, :] * X[s, g, r + 1, pl.ds(PAD - EXT + c + 1, COLS), :]
                new = new + C[2, r, cat, :] * X[s, g, r + 1, pl.ds(PAD - EXT + c - 1, COLS), :]
                if flag is not None:
                    new = new + jnp.where(flag, Y[total + 1, g, r + 1, at, :], 0.0)
                X[s + 1, g, r + 1, at, :] = new

    def turn(X, C, m, s, g, flag=None):
        @pl.when(s == 0)
        def _():
            wait_rows(lambda: row_up(X, m, g), lambda: row_down(X, m, g))

        @pl.when(s > 0)
        def _():
            wait_rows(lambda: lat_up(X, m, s, g), lambda: lat_down(X, m, s, g))

        advance(X, C, s, g, flag)

        if flag is None:
            @pl.when(s < kept)
            def _():
                for r in range(rows):
                    H[total + 1, g, r + 1, own, :] = jnp.where(
                        s < first_count, H[s + 1, g, r + 1, own, :], H[total + 1, g, r + 1, own, :])

        @pl.when(s < total - 1)
        def _():
            start_up_down([lambda: lat_up(X, m, s + 1, g)], [lambda: lat_down(X, m, s + 1, g)])

    def wait_edges(X, n, m, diagonals=True):
        for copy in lon_halo(X, n, m):
            copy.wait_recv()
        if diagonals:
            @pl.when(has_down)
            def _():
                for n in range(2):
                    diag_up(X, m, n).wait_recv()

            @pl.when(has_up)
            def _():
                for n in range(2):
                    diag_down(X, m, n).wait_recv()

    earlier = lax.broadcasted_iota(jnp.int32, (soundings, soundings), 0) < lax.broadcasted_iota(
        jnp.int32, (soundings, soundings), 1)

    def observe(k):
        @pl.loop(1, devices)
        def _(j):
            hand_over(k, j).wait_recv()

        placed = one_hot(cell_ref[pl.ds(k, 1), :], cells)
        owner = owner_ref[k]
        spread = jnp.broadcast_to(owner.astype(jnp.float32), (soundings, soundings))
        same = jnp.logical_and(spread.T == spread, earlier)
        rank = jnp.sum(same.astype(jnp.float32), axis=0, keepdims=True).astype(jnp.int32)
        places = block // chunks
        source = one_hot(owner * places + rank, devices * places)
        wanted = []
        for h in range(chunks):
            got = dot(source, jnp.concatenate(split2(GOT[k, pl.ds(h, devices * places, stride=chunks), :]), axis=1), FIRST)
            wanted.append(got[:, :LANES] + got[:, LANES:])
        wanted = jnp.concatenate(wanted, axis=1)
        weight = jnp.concatenate([WS[b:b + 1, :] for b in range(chunks)], axis=1)
        high, low = [], []
        for g in range(groups):
            field = H[total + 1 - k, g, inner, own, :].reshape(cells, LANES)
            taken = dot(placed, jnp.concatenate(split2(field), axis=1), FIRST).astype(jnp.bfloat16)
            high.append(taken[:, :LANES])
            low.append(taken[:, LANES:])
        high = jnp.concatenate(high, axis=1)
        low = jnp.concatenate(low, axis=1)
        table, rest = AE[:, pl.ds(0, prof)], AE[:, pl.ds(prof, prof)]
        both = dot(jnp.concatenate([high, low], axis=0), table, LAST)
        both = both[:soundings] + both[soundings:] + dot(high, rest, LAST)
        optical, bright = both[:, :used], both[:, used:]
        small = jnp.exp(-jnp.abs(optical))
        inv = 1.0 / (1.0 + small)
        passed = jnp.where(optical > 0, small, 1.0) * inv
        slope = jnp.where(optical > 0, 1.0, small) * inv
        y = passed * bright
        departure = weight * (y - wanted)
        high, low = split2(jnp.concatenate([-(departure * y) * slope, departure * passed], axis=1))
        both = dot(jnp.concatenate([high, low], axis=0), table)
        back = both[:soundings] + both[soundings:] + dot(high, rest)
        back = jnp.concatenate(split2(back), axis=0)
        placed = jnp.concatenate([placed, placed], axis=1)
        target = jnp.where(k == 0, total + 1, 0)
        for g in range(groups):
            Y[target, g, inner, own, :] = dot(placed, back[:, g * LANES:(g + 1) * LANES]).reshape(rows, width, LANES)

            @pl.when(k > 0)
            def _():
                start_up_down([lambda: row_up(Y, 1, g)], [lambda: row_down(Y, 1, g)])

        for copy in lon_halo(Y, target, 2 - k):
            copy.start()

        @pl.when(k > 0)
        def _():
            start_up_down([partial(diag_up, Y, 1, n) for n in range(2)], [partial(diag_down, Y, 1, n) for n in range(2)])

    wait_edges(H, 0, 0)
    turns = total * groups
    handed = slots * (devices - 1)
    share = -(-handed // turns)
    early = kept * groups - 1

    @pl.loop(0, turns + 1)
    def _(it):
        @pl.loop(it * share, jnp.minimum((it + 1) * share, handed))
        def _(n):
            hand_over(n // (devices - 1), 1 + n % (devices - 1)).start()

        @pl.when(it < turns)
        def _():
            turn(H, F, 0, it // groups, it % groups)

        @pl.when(jnp.logical_or(it == early, it == turns))
        def _():
            observe((it == turns).astype(jnp.int32))

    wait_edges(Y, 0, 1)
    wait_edges(Y, total + 1, 2, diagonals=False)

    @pl.loop(0, turns)
    def _(it):
        s = it // groups
        g = it % groups
        turn(Y, B, 1, s, g, s + 1 == second_count)

        @pl.when(s == total - 1)
        def _():
            for r in range(rows):
                out_ref[pl.ds(g * LANES * rows + r, LANES, stride=rows), :] = Y[total, g, r + 1, own, :].T

    for copy in pk_lon():
        copy.wait_send()
    for X, n, m in ((H, 0, 0), (Y, 0, 1), (Y, total + 1, 2)):
        for copy in lon_halo(X, n, m):
            copy.wait_send()

    @pl.when(has_down)
    def _():
        for n in range(3):
            pk_down(n).wait_send()

    for X, m in ((H, 0), (Y, 1)):
        @pl.when(has_up)
        def _():
            for n in range(2):
                diag_up(X, m, n).wait_send()

            @pl.loop(0, groups)
            def _(g):
                row_up(X, m, g).wait_send()

            @pl.loop(groups, turns)
            def _(n):
                lat_up(X, m, n // groups, n % groups).wait_send()

        @pl.when(has_down)
        def _():
            for n in range(2):
                diag_down(X, m, n).wait_send()

            @pl.loop(0, groups)
            def _(g):
                row_down(X, m, g).wait_send()

            @pl.loop(groups, turns)
            def _(n):
                lat_down(X, m, n // groups, n % groups).wait_send()

    @pl.loop(0, handed)
    def _(n):
        hand_over(n // (devices - 1), 1 + n % (devices - 1)).wait_send()


def whole_call(lat_count, lon_count, total, step_counts, state, winds, diffusivity, by_rank, absorb, emit,
               cells, owners, channel_list, weight):
    rows, width = diffusivity.shape
    groups = state.shape[0] // (rows * LANES)
    slots, capacity, devices, used = by_rank.shape
    channels, prof = absorb.shape
    block = -(-capacity * (used // LANES) // 8) * 8
    wide = width + 2 * PAD
    span = width + 2 * EXT
    vmem = pl.BlockSpec(memory_space=pltpu.VMEM)
    hbm = pl.BlockSpec(memory_space=pl.ANY)
    f32, bf16 = jnp.float32, jnp.bfloat16
    dma = pltpu.SemaphoreType.DMA
    scratch = [
        pltpu.VMEM(state.shape, f32), pltpu.VMEM(winds.shape, f32), pltpu.VMEM(diffusivity.shape, f32),
        pltpu.VMEM(by_rank.shape, f32), pltpu.VMEM((2, channels, prof), f32),
        pltpu.VMEM((2, channels, 2 * prof), bf16), pltpu.VMEM((2 * used, 2 * prof), bf16),
        pltpu.VMEM((used // LANES, LANES), f32),
        pltpu.VMEM((total + 2, groups, rows + 2, wide, LANES), f32),
        pltpu.VMEM((total + 2, groups, rows + 2, wide, LANES), f32),
        pltpu.VMEM((5, rows, span, LANES), f32), pltpu.VMEM((5, rows, span, LANES), f32),
        pltpu.VMEM((2, rows, wide, LANES), f32), pltpu.VMEM((wide, LANES), f32),
        pltpu.VMEM((slots, devices * block, LANES), f32), pltpu.VMEM((slots, devices * block, LANES), f32),
        dma((6,)), dma((5,)), dma((5,)), dma((2, groups, 2)), dma((2, groups, 2)), dma((3, 2)), dma((3, 2)),
        dma((2, 4)), dma((2, 4)), dma((2, total, groups, 2)), dma((2, total, groups, 2)),
        dma((slots, devices)), dma((slots, devices)),
    ]
    return pl.pallas_call(
        partial(whole_kernel, total, lat_count, lon_count),
        out_shape=jax.ShapeDtypeStruct(state.shape, f32),
        in_specs=[pl.BlockSpec(memory_space=pltpu.SMEM)] + [hbm] * 6 + [vmem] * 4,
        out_specs=vmem,
        scratch_shapes=scratch,
        compiler_params=pltpu.CompilerParams(
            collective_id=total, has_side_effects=True, vmem_limit_bytes=60 << 20),
        name="whole",
    )(step_counts, state, winds, diffusivity, by_rank, absorb, emit, cells, owners, channel_list, weight)


def per_device(lat_count, lon_count, state, winds, diffusivity, sounding_cell, sounding_owner,
               step_counts, channel_list, absorb_table, emit_table, obs_weight, observed):
    width = state.shape[-1]
    operands = (
        step_counts, state.reshape(-1, width), winds.reshape(-1, width), diffusivity,
        jnp.transpose(observed[:, 0], (0, 2, 1, 3)), absorb_table.T, emit_table.T,
        sounding_cell, jnp.transpose(sounding_owner, (0, 2, 1)), channel_list.reshape(-1, LANES),
        obs_weight[None, :])
    slots = step_counts.shape[0]
    branches = [partial(whole_call, lat_count, lon_count, n) for n in range(slots, slots * MAXSTEP + 1)]
    return lax.switch(step_counts[0] + step_counts[1] - slots, branches, *operands).reshape(state.shape)


def solution(mesh):
    return jax.shard_map(
        partial(per_device, mesh.shape["lat"], mesh.shape["lon"]),
        mesh=mesh,
        in_specs=(
            P(None, None, "lat", "lon"),
            P(None, None, "lat", "lon"),
            P("lat", "lon"),
            P(None, ("lon", "lat")),
            P(None, ("lon", "lat"), None),
            P(),
            P(),
            P(),
            P(),
            P(),
            P(None, ("lon", "lat"), None, None, None),
        ),
        out_specs=P(None, None, "lat", "lon"),
        check_vma=False,
    )
```

```python
from functools import partial

import jax
import jax.numpy as jnp
from jax import lax
from jax.experimental import pallas as pl
from jax.experimental.pallas import tpu as pltpu
from jax.sharding import PartitionSpec as P

MAXSTEP = 4
LANES = 128
EXT = 8
PAD = 16
COLS = 24
MESH_ID = pl.DeviceIdType.MESH
FIRST = ((0,), (0,))
LAST = ((1,), (1,))


def split2(v):
    high = v.astype(jnp.bfloat16)
    return high, (v - high.astype(jnp.float32)).astype(jnp.bfloat16)


def split3(v):
    high = v.astype(jnp.bfloat16)
    rest = v - high.astype(jnp.float32)
    mid = rest.astype(jnp.bfloat16)
    return high, mid, (rest - mid.astype(jnp.float32)).astype(jnp.bfloat16)


def dot(a, b, dims=((1,), (0,))):
    return lax.dot_general(a, b, (dims, ((), ())), preferred_element_type=jnp.float32)


def one_hot(row, size):
    return (row == lax.broadcasted_iota(jnp.int32, (size, row.shape[1]), 0)).astype(
        jnp.float32).astype(jnp.bfloat16)


def whole_kernel(total, lat_count, lon_count, *refs):
    (steps_ref, state_hbm, winds_hbm, diff_hbm, obs_hbm, absorb_hbm, emit_hbm, cell_ref, owner_ref, chan_ref,
     weight_ref, out_ref,
     state, winds, diff, obs, tables, TB, AE, WS, H, Y, F, B, PK, SB, GOT,
     local_sem, pk_s, pk_r, row_s, row_r, lon_s, lon_r, diag_s, diag_r, lat_s, lat_r, obs_s, obs_r) = refs
    groups, rows = H.shape[1], H.shape[2] - 2
    width = state.shape[1]
    span = width + 2 * EXT
    levels = winds.shape[0] // (2 * rows)
    devices = lat_count * lon_count
    slots, capacity, _, used = obs.shape
    chunks = used // LANES
    block = SB.shape[1] // devices
    channels, prof = tables.shape[1:]
    cells = rows * width
    soundings = cell_ref.shape[1]
    lat = lax.axis_index("lat")
    lon = lax.axis_index("lon")
    me = lon * lat_count + lat
    east = lax.rem(lon + 1, lon_count)
    west = lax.rem(lon + lon_count - 1, lon_count)
    has_up = lat > 0
    has_down = lat < lat_count - 1
    up, down = lat - 1, lat + 1
    own = pl.ds(PAD, width)
    wide = pl.ds(PAD - EXT, span)
    head, tail = pl.ds(PAD, EXT), pl.ds(PAD + width - EXT, EXT)
    before, after = pl.ds(PAD - EXT, EXT), pl.ds(PAD + width, EXT)
    inner = pl.ds(1, rows)
    top, bottom, above, below = 1, rows, 0, rows + 1

    loads = [pltpu.make_async_copy(src, dst, local_sem.at[n]) for n, (src, dst) in enumerate((
        (state_hbm, state), (winds_hbm, winds), (diff_hbm, diff), (obs_hbm, obs),
        (absorb_hbm, tables.at[0]), (emit_hbm, tables.at[1])))]
    for load in loads[:4]:
        load.start()
    barrier = pltpu.get_barrier_semaphore()

    @pl.loop(1, devices)
    def _(j):
        other = (me + j) % devices
        pl.semaphore_signal(barrier, inc=1, device_id={"lon": other // lat_count, "lat": other % lat_count},
                            device_id_type=MESH_ID)

    def remote(src, dst, s, r, to_lat, to_lon):
        return pltpu.make_async_remote_copy(
            src, dst, s, r, device_id={"lon": to_lon, "lat": to_lat}, device_id_type=MESH_ID)

    middle = lon_count // 2 * lat_count

    def hand_over(k, n):
        shift = n + n // middle
        to_lon = lax.rem(lon + lon_count // 2 + shift // lat_count, lon_count)
        to_lat = lax.rem(lat + shift % lat_count, lat_count)
        other = to_lon * lat_count + to_lat
        return remote(SB.at[k, pl.ds(other * block, block)], GOT.at[k, pl.ds(me * block, block)],
                      obs_s.at[k, n], obs_r.at[k, n], to_lat, to_lon)

    def pk_lon():
        return (remote(PK.at[:, inner, tail], PK.at[:, inner, before], pk_s.at[0], pk_r.at[0], lat, east),
                remote(PK.at[:, inner, head], PK.at[:, inner, after], pk_s.at[1], pk_r.at[1], lat, west))

    def pk_down(n):
        src, dst, to_lon = ((own, own, lon), (tail, before, east), (head, after, west))[n]
        return remote(PK.at[1, rows, src], PK.at[1, 0, dst], pk_s.at[2 + n], pk_r.at[2 + n], down, to_lon)

    def lon_halo(X, n, m):
        return (remote(X.at[n, :, inner, tail], X.at[n, :, inner, before], lon_s.at[m, 0], lon_r.at[m, 0], lat, east),
                remote(X.at[n, :, inner, head], X.at[n, :, inner, after], lon_s.at[m, 1], lon_r.at[m, 1], lat, west))

    def diag_up(X, m, n):
        src, dst, to_lon = ((tail, before, east), (head, after, west))[n]
        return remote(X.at[0, :, top, src], X.at[0, :, below, dst], diag_s.at[m, n], diag_r.at[m, n], up, to_lon)

    def diag_down(X, m, n):
        src, dst, to_lon = ((tail, before, east), (head, after, west))[n]
        return remote(X.at[0, :, bottom, src], X.at[0, :, above, dst], diag_s.at[m, 2 + n], diag_r.at[m, 2 + n],
                      down, to_lon)

    def row_up(X, m, g):
        return remote(X.at[0, g, top, own], X.at[0, g, below, own], row_s.at[m, g, 0], row_r.at[m, g, 0], up, lon)

    def row_down(X, m, g):
        return remote(X.at[0, g, bottom, own], X.at[0, g, above, own], row_s.at[m, g, 1], row_r.at[m, g, 1], down, lon)

    margin = total - 2
    some = pl.ds(PAD - margin, width + 2 * margin)

    def lat_up(X, m, s, g):
        return remote(X.at[s, g, top, some], X.at[s, g, below, some], lat_s.at[m, s, g, 0], lat_r.at[m, s, g, 0], up, lon)

    def lat_down(X, m, s, g):
        return remote(X.at[s, g, bottom, some], X.at[s, g, above, some], lat_s.at[m, s, g, 1], lat_r.at[m, s, g, 1],
                      down, lon)

    def start_up_down(upward, downward):
        @pl.when(has_up)
        def _():
            for copy in upward:
                copy().start()

        @pl.when(has_down)
        def _():
            for copy in downward:
                copy().start()

    def start_diagonals(X, m):
        start_up_down([partial(diag_up, X, m, n) for n in range(2)], [partial(diag_down, X, m, n) for n in range(2)])

    def wait_rows(upward, downward):
        @pl.when(has_down)
        def _():
            upward().wait_recv()
            downward().wait_send()

        @pl.when(has_up)
        def _():
            downward().wait_recv()
            upward().wait_send()

    loads[0].wait()

    @pl.loop(0, groups)
    def _(g):
        for r in range(rows):
            H[0, g, r + 1, own, :] = state[pl.ds(g * LANES * rows + r, LANES, stride=rows), :].T

    loads[1].wait()
    loads[2].wait()
    for i in range(2):
        for r in range(rows):
            w = winds[pl.ds(i * levels * rows + r, levels, stride=rows), :] * 0.5
            d = diff[pl.ds(r, 1), :]
            PK[i, r + 1, own, :] = jnp.concatenate([w + d, w - d], axis=0).T

    edge = jnp.zeros((span, LANES), jnp.float32)

    @pl.when(jnp.logical_not(has_up))
    def _():
        PK[1, 0, wide, :] = edge

        @pl.loop(0, total * groups)
        def _(n):
            for X in (H, Y):
                X[n // groups, n % groups, above, wide, :] = edge

    @pl.when(jnp.logical_not(has_down))
    def _():
        @pl.loop(0, total * groups)
        def _(n):
            for X in (H, Y):
                X[n // groups, n % groups, below, wide, :] = edge

    pl.semaphore_wait(barrier, devices - 1)

    for copy in pk_lon():
        copy.start()
    start_up_down((), [partial(pk_down, n) for n in range(3)])
    for copy in lon_halo(H, 0, 0):
        copy.start()
    start_diagonals(H, 0)

    @pl.loop(0, groups)
    def _(g):
        start_up_down([lambda: row_up(H, 0, g)], [lambda: row_down(H, 0, g)])

    for load in loads[4:]:
        load.start()
    loads[3].wait()

    @pl.loop(0, slots)
    def _(k):
        for c in range(capacity):
            for h in range(chunks):
                SB[k, pl.ds(c * chunks + h, devices, stride=block), :] = obs[k, c, :, pl.ds(h * LANES, LANES)]
        for c in range(capacity * chunks, block):
            SB[k, pl.ds(c, devices, stride=block), :] = jnp.zeros((devices, LANES), jnp.float32)
        GOT[k, pl.ds(me * block, block), :] = SB[k, pl.ds(me * block, block), :]

    @pl.loop(0, slots * (devices - 1))
    def _(n):
        hand_over(n // (devices - 1), n % (devices - 1)).start()

    loads[4].wait()
    loads[5].wait()
    part = channels // 7

    @pl.loop(0, 14)
    def _(n):
        at = pl.ds(n % 7 * part, part)
        high, low = split2(tables[n // 7, at, :])
        TB[n // 7, at, pl.ds(0, prof)] = high
        TB[n // 7, at, pl.ds(prof, prof)] = low

    weights = jnp.concatenate([jnp.broadcast_to(v, (8, channels)) for v in split3(weight_ref[...].reshape(1, channels))], axis=0)

    @pl.loop(0, chunks)
    def _(b):
        column = jnp.broadcast_to(chan_ref[pl.ds(b, 1), :].astype(jnp.float32), (LANES, LANES)).T
        column = jnp.concatenate([column] * -(-channels // LANES), axis=1)[:, :channels]
        picker = (column == lax.broadcasted_iota(jnp.int32, (LANES, channels), 1).astype(jnp.float32)).astype(
            jnp.float32).astype(jnp.bfloat16)
        w = dot(weights, picker, LAST)
        WS[pl.ds(b, 1), :] = w[0:1] + w[8:9] + w[16:17]

        @pl.loop(0, 2)
        def _(t):
            AE[pl.ds(t * used + b * LANES, LANES), :] = dot(picker, TB[t]).astype(jnp.bfloat16)

    for copy in pk_lon():
        copy.wait_recv()

    @pl.when(has_up)
    def _():
        for n in range(3):
            pk_down(n).wait_recv()

    lower = lax.broadcasted_iota(jnp.int32, (span, LANES), 1) < levels

    def unpack(v):
        other = pltpu.roll(v, levels, 1)
        return jnp.where(lower, v, other), jnp.where(lower, other, v)

    @pl.loop(0, rows)
    def _(r):
        a, b = unpack(PK[0, r + 1, wide, :])
        aw, bw = unpack(PK[0, r + 1, pl.ds(PAD - EXT - 1, span), :])
        al, bl = unpack(PK[1, r + 1, wide, :])
        au, bu = unpack(PK[1, r, wide, :])
        centre = 1.0 - a + bw - al + bu
        for n, v in enumerate((centre, -b, aw, -bl, au)):
            F[n, r] = v
        for n, v in enumerate((centre, a, -bw, al, -bu)):
            B[n, r] = v

    first_count = steps_ref[0]
    second_count = steps_ref[1]
    kept = min(MAXSTEP, total - 1)

    def advance(X, C, s, g, flag=None):
        for c in range(0, span, COLS):
            at = pl.ds(PAD - EXT + c, COLS)
            cat = pl.ds(c, COLS)
            row = [X[s, g, r, at, :] for r in range(rows + 2)]
            for r in range(rows):
                new = C[0, r, cat, :] * row[r + 1]
                new = new + C[3, r, cat, :] * row[r + 2]
                new = new + C[4, r, cat, :] * row[r]
                new = new + C[1, r, cat, :] * X[s, g, r + 1, pl.ds(PAD - EXT + c + 1, COLS), :]
                new = new + C[2, r, cat, :] * X[s, g, r + 1, pl.ds(PAD - EXT + c - 1, COLS), :]
                if flag is not None:
                    new = new + jnp.where(flag, Y[total + 1, g, r + 1, at, :], 0.0)
                X[s + 1, g, r + 1, at, :] = new

    def turn(X, C, m, s, g, flag=None):
        @pl.when(s == 0)
        def _():
            wait_rows(lambda: row_up(X, m, g), lambda: row_down(X, m, g))

        @pl.when(s > 0)
        def _():
            wait_rows(lambda: lat_up(X, m, s, g), lambda: lat_down(X, m, s, g))

        advance(X, C, s, g, flag)

        if flag is None:
            @pl.when(s < kept)
            def _():
                for r in range(rows):
                    H[total + 1, g, r + 1, own, :] = jnp.where(
                        s < first_count, H[s + 1, g, r + 1, own, :], H[total + 1, g, r + 1, own, :])

        @pl.when(s < total - 1)
        def _():
            start_up_down([lambda: lat_up(X, m, s + 1, g)], [lambda: lat_down(X, m, s + 1, g)])

    def wait_edges(X, n, m, diagonals=True):
        for copy in lon_halo(X, n, m):
            copy.wait()
        if diagonals:
            @pl.when(has_down)
            def _():
                for n in range(2):
                    diag_up(X, m, n).wait_recv()
                    diag_down(X, m, n).wait_send()

            @pl.when(has_up)
            def _():
                for n in range(2):
                    diag_down(X, m, n).wait_recv()
                    diag_up(X, m, n).wait_send()

    earlier = lax.broadcasted_iota(jnp.int32, (soundings, soundings), 0) < lax.broadcasted_iota(
        jnp.int32, (soundings, soundings), 1)

    def observe(k):
        @pl.loop(0, devices - 1)
        def _(n):
            hand_over(k, n).wait_recv()

        placed = one_hot(cell_ref[pl.ds(k, 1), :], cells)
        owner = owner_ref[k]
        spread = jnp.broadcast_to(owner.astype(jnp.float32), (soundings, soundings))
        same = jnp.logical_and(spread.T == spread, earlier)
        rank = jnp.sum(same.astype(jnp.float32), axis=0, keepdims=True).astype(jnp.int32)
        places = block // chunks
        source = one_hot(owner * places + rank, devices * places)
        wanted = []
        for h in range(chunks):
            got = dot(source, jnp.concatenate(split2(GOT[k, pl.ds(h, devices * places, stride=chunks), :]), axis=1), FIRST)
            wanted.append(got[:, :LANES] + got[:, LANES:])
        wanted = jnp.concatenate(wanted, axis=1)
        weight = jnp.concatenate([WS[b:b + 1, :] for b in range(chunks)], axis=1)
        high, low = [], []
        for g in range(groups):
            field = H[total + 1 - k, g, inner, own, :].reshape(cells, LANES)
            taken = dot(placed, jnp.concatenate(split2(field), axis=1), FIRST).astype(jnp.bfloat16)
            high.append(taken[:, :LANES])
            low.append(taken[:, LANES:])
        high = jnp.concatenate(high, axis=1)
        low = jnp.concatenate(low, axis=1)
        table, rest = AE[:, pl.ds(0, prof)], AE[:, pl.ds(prof, prof)]
        both = dot(jnp.concatenate([high, low], axis=0), table, LAST)
        both = both[:soundings] + both[soundings:] + dot(high, rest, LAST)
        optical, bright = both[:, :used], both[:, used:]
        small = jnp.exp(-jnp.abs(optical))
        inv = 1.0 / (1.0 + small)
        passed = jnp.where(optical > 0, small, 1.0) * inv
        slope = jnp.where(optical > 0, 1.0, small) * inv
        y = passed * bright
        departure = weight * (y - wanted)
        high, low = split2(jnp.concatenate([-(departure * y) * slope, departure * passed], axis=1))
        both = dot(jnp.concatenate([high, low], axis=0), table)
        back = both[:soundings] + both[soundings:] + dot(high, rest)
        back = jnp.concatenate(split2(back), axis=0)
        placed = jnp.concatenate([placed, placed], axis=1)
        target = jnp.where(k == 0, total + 1, 0)
        for g in range(groups):
            Y[target, g, inner, own, :] = dot(placed, back[:, g * LANES:(g + 1) * LANES]).reshape(rows, width, LANES)

        for copy in lon_halo(Y, target, 2 - k):
            copy.start()

        @pl.when(k > 0)
        def _():
            start_diagonals(Y, 1)

            @pl.loop(0, groups)
            def _(g):
                start_up_down([lambda: row_up(Y, 1, g)], [lambda: row_down(Y, 1, g)])

    wait_edges(H, 0, 0)
    turns = total * groups
    early = kept * groups - 1

    @pl.loop(0, turns + 1)
    def _(it):
        @pl.when(it < turns)
        def _():
            turn(H, F, 0, it // groups, it % groups)

        @pl.when(jnp.logical_or(it == early, it == turns))
        def _():
            observe((it == turns).astype(jnp.int32))

    @pl.loop(0, slots * (devices - 1))
    def _(n):
        hand_over(n // (devices - 1), n % (devices - 1)).wait_send()

    for copy in pk_lon():
        copy.wait_send()

    @pl.when(has_down)
    def _():
        for n in range(3):
            pk_down(n).wait_send()

    wait_edges(Y, 0, 1)
    wait_edges(Y, total + 1, 2, diagonals=False)

    @pl.loop(0, turns)
    def _(it):
        s = it // groups
        g = it % groups
        turn(Y, B, 1, s, g, s + 1 == second_count)

        @pl.when(s == total - 1)
        def _():
            for r in range(rows):
                out_ref[pl.ds(g * LANES * rows + r, LANES, stride=rows), :] = Y[total, g, r + 1, own, :].T


def whole_call(lat_count, lon_count, total, step_counts, state, winds, diffusivity, by_rank, absorb, emit,
               cells, owners, channel_list, weight):
    rows, width = diffusivity.shape
    groups = state.shape[0] // (rows * LANES)
    slots, capacity, devices, used = by_rank.shape
    channels, prof = absorb.shape
    block = -(-capacity * (used // LANES) // 8) * 8
    wide = width + 2 * PAD
    span = width + 2 * EXT
    vmem = pl.BlockSpec(memory_space=pltpu.VMEM)
    hbm = pl.BlockSpec(memory_space=pl.ANY)
    f32, bf16 = jnp.float32, jnp.bfloat16
    dma = pltpu.SemaphoreType.DMA
    scratch = [
        pltpu.VMEM(state.shape, f32), pltpu.VMEM(winds.shape, f32), pltpu.VMEM(diffusivity.shape, f32),
        pltpu.VMEM(by_rank.shape, f32), pltpu.VMEM((2, channels, prof), f32),
        pltpu.VMEM((2, channels, 2 * prof), bf16), pltpu.VMEM((2 * used, 2 * prof), bf16),
        pltpu.VMEM((used // LANES, LANES), f32),
        pltpu.VMEM((total + 2, groups, rows + 2, wide, LANES), f32),
        pltpu.VMEM((total + 2, groups, rows + 2, wide, LANES), f32),
        pltpu.VMEM((5, rows, span, LANES), f32), pltpu.VMEM((5, rows, span, LANES), f32),
        pltpu.VMEM((2, rows + 1, wide, LANES), f32),
        pltpu.VMEM((slots, devices * block, LANES), f32), pltpu.VMEM((slots, devices * block, LANES), f32),
        dma((6,)), dma((5,)), dma((5,)), dma((2, groups, 2)), dma((2, groups, 2)), dma((3, 2)), dma((3, 2)),
        dma((2, 4)), dma((2, 4)), dma((2, total, groups, 2)), dma((2, total, groups, 2)),
        dma((slots, devices)), dma((slots, devices)),
    ]
    return pl.pallas_call(
        partial(whole_kernel, total, lat_count, lon_count),
        out_shape=jax.ShapeDtypeStruct(state.shape, f32),
        in_specs=[pl.BlockSpec(memory_space=pltpu.SMEM)] + [hbm] * 6 + [vmem] * 4,
        out_specs=vmem,
        scratch_shapes=scratch,
        compiler_params=pltpu.CompilerParams(
            collective_id=total, has_side_effects=True, vmem_limit_bytes=60 << 20),
        name="whole",
    )(step_counts, state, winds, diffusivity, by_rank, absorb, emit, cells, owners, channel_list, weight)


def per_device(lat_count, lon_count, state, winds, diffusivity, sounding_cell, sounding_owner,
               step_counts, channel_list, absorb_table, emit_table, obs_weight, observed):
    width = state.shape[-1]
    operands = (
        step_counts, state.reshape(-1, width), winds.reshape(-1, width), diffusivity,
        jnp.transpose(observed[:, 0], (0, 2, 1, 3)), absorb_table.T, emit_table.T,
        sounding_cell, jnp.transpose(sounding_owner, (0, 2, 1)), channel_list.reshape(-1, LANES),
        obs_weight)
    slots = step_counts.shape[0]
    branches = [partial(whole_call, lat_count, lon_count, n) for n in range(slots, slots * MAXSTEP + 1)]
    return lax.switch(step_counts[0] + step_counts[1] - slots, branches, *operands).reshape(state.shape)


def solution(mesh):
    return jax.shard_map(
        partial(per_device, mesh.shape["lat"], mesh.shape["lon"]),
        mesh=mesh,
        in_specs=(
            P(None, None, "lat", "lon"),
            P(None, None, "lat", "lon"),
            P("lat", "lon"),
            P(None, ("lon", "lat")),
            P(None, ("lon", "lat"), None),
            P(),
            P(),
            P(),
            P(),
            P(),
            P(None, ("lon", "lat"), None, None, None),
        ),
        out_specs=P(None, None, "lat", "lon"),
        check_vma=False,
    )
```

```python
from functools import partial

import jax
import jax.numpy as jnp
from jax import lax
from jax.experimental import pallas as pl
from jax.experimental.pallas import tpu as pltpu
from jax.sharding import PartitionSpec as P

MAXSTEP = 4
LANES = 128
EXT = 8
PAD = 16
COLS = 24
MESH_ID = pl.DeviceIdType.MESH
FIRST = ((0,), (0,))
LAST = ((1,), (1,))


def split2(v):
    high = v.astype(jnp.bfloat16)
    return high, (v - high.astype(jnp.float32)).astype(jnp.bfloat16)


def split3(v):
    high = v.astype(jnp.bfloat16)
    rest = v - high.astype(jnp.float32)
    mid = rest.astype(jnp.bfloat16)
    return high, mid, (rest - mid.astype(jnp.float32)).astype(jnp.bfloat16)


def dot(a, b, dims=((1,), (0,))):
    return lax.dot_general(a, b, (dims, ((), ())), preferred_element_type=jnp.float32)


def one_hot(row, size):
    return (row == lax.broadcasted_iota(jnp.int32, (size, row.shape[1]), 0)).astype(
        jnp.float32).astype(jnp.bfloat16)


def whole_kernel(total, lat_count, lon_count, *refs):
    (steps_ref, state_hbm, winds_hbm, diff_hbm, obs_hbm, absorb_hbm, emit_hbm, cell_ref, owner_ref, chan_ref,
     weight_ref, out_ref,
     state, winds, diff, obs, tables, TB, AE, WS, H, Y, F, B, PK, SB, GOT, WN,
     local_sem, state_sem, pk_s, pk_r, row_s, row_r, lon_s, lon_r, diag_s, diag_r, lat_s, lat_r, obs_s, obs_r) = refs
    groups, rows = H.shape[1], H.shape[2] - 2
    width = state.shape[1]
    span = width + 2 * EXT
    levels = winds.shape[0] // (2 * rows)
    devices = lat_count * lon_count
    slots, capacity, _, used = obs.shape
    chunks = used // LANES
    block = SB.shape[1] // devices
    channels, prof = tables.shape[1:]
    cells = rows * width
    soundings = cell_ref.shape[1]
    lat = lax.axis_index("lat")
    lon = lax.axis_index("lon")
    me = lon * lat_count + lat
    east = lax.rem(lon + 1, lon_count)
    west = lax.rem(lon + lon_count - 1, lon_count)
    has_up = lat > 0
    has_down = lat < lat_count - 1
    up, down = lat - 1, lat + 1
    own = pl.ds(PAD, width)
    wide = pl.ds(PAD - EXT, span)
    head, tail = pl.ds(PAD, EXT), pl.ds(PAD + width - EXT, EXT)
    before, after = pl.ds(PAD - EXT, EXT), pl.ds(PAD + width, EXT)
    inner = pl.ds(1, rows)
    top, bottom, above, below = 1, rows, 0, rows + 1

    loads = [pltpu.make_async_copy(src, dst, local_sem.at[n]) for n, (src, dst) in enumerate((
        (winds_hbm, winds), (diff_hbm, diff), (obs_hbm, obs),
        (absorb_hbm, tables.at[0]), (emit_hbm, tables.at[1])))]
    for load in loads[:2]:
        load.start()

    def state_load(g):
        at = pl.ds(g * LANES * rows, LANES * rows)
        return pltpu.make_async_copy(state_hbm.at[at], state.at[at], state_sem.at[g])

    @pl.loop(0, groups)
    def _(g):
        state_load(g).start()

    loads[2].start()
    barrier = pltpu.get_barrier_semaphore()

    @pl.loop(1, devices)
    def _(j):
        other = (me + j) % devices
        pl.semaphore_signal(barrier, inc=1, device_id={"lon": other // lat_count, "lat": other % lat_count},
                            device_id_type=MESH_ID)

    def remote(src, dst, s, r, to_lat, to_lon):
        return pltpu.make_async_remote_copy(
            src, dst, s, r, device_id={"lon": to_lon, "lat": to_lat}, device_id_type=MESH_ID)

    middle = lon_count // 2 * lat_count

    def hand_over(k, n):
        shift = n + n // middle
        to_lon = lax.rem(lon + lon_count // 2 + shift // lat_count, lon_count)
        to_lat = lax.rem(lat + shift % lat_count, lat_count)
        other = to_lon * lat_count + to_lat
        return remote(SB.at[k, pl.ds(other * block, block)], GOT.at[k, pl.ds(me * block, block)],
                      obs_s.at[k, n], obs_r.at[k, n], to_lat, to_lon)

    def pk_lon():
        return (remote(PK.at[:, inner, tail], PK.at[:, inner, before], pk_s.at[0], pk_r.at[0], lat, east),
                remote(PK.at[:, inner, head], PK.at[:, inner, after], pk_s.at[1], pk_r.at[1], lat, west))

    def pk_down(n):
        src, dst, to_lon = ((own, own, lon), (tail, before, east), (head, after, west))[n]
        return remote(PK.at[1, rows, src], PK.at[1, 0, dst], pk_s.at[2 + n], pk_r.at[2 + n], down, to_lon)

    def lon_halo(X, n, m):
        return (remote(X.at[n, :, inner, tail], X.at[n, :, inner, before], lon_s.at[m, 0], lon_r.at[m, 0], lat, east),
                remote(X.at[n, :, inner, head], X.at[n, :, inner, after], lon_s.at[m, 1], lon_r.at[m, 1], lat, west))

    def diag_up(X, m, n):
        src, dst, to_lon = ((tail, before, east), (head, after, west))[n]
        return remote(X.at[0, :, top, src], X.at[0, :, below, dst], diag_s.at[m, n], diag_r.at[m, n], up, to_lon)

    def diag_down(X, m, n):
        src, dst, to_lon = ((tail, before, east), (head, after, west))[n]
        return remote(X.at[0, :, bottom, src], X.at[0, :, above, dst], diag_s.at[m, 2 + n], diag_r.at[m, 2 + n],
                      down, to_lon)

    def row_up(X, m, g):
        return remote(X.at[0, g, top, own], X.at[0, g, below, own], row_s.at[m, g, 0], row_r.at[m, g, 0], up, lon)

    def row_down(X, m, g):
        return remote(X.at[0, g, bottom, own], X.at[0, g, above, own], row_s.at[m, g, 1], row_r.at[m, g, 1], down, lon)

    margin = total - 2
    some = pl.ds(PAD - margin, width + 2 * margin)

    def lat_up(X, m, s, g):
        return remote(X.at[s, g, top, some], X.at[s, g, below, some], lat_s.at[m, s, g, 0], lat_r.at[m, s, g, 0], up, lon)

    def lat_down(X, m, s, g):
        return remote(X.at[s, g, bottom, some], X.at[s, g, above, some], lat_s.at[m, s, g, 1], lat_r.at[m, s, g, 1],
                      down, lon)

    def start_up_down(upward, downward):
        @pl.when(has_up)
        def _():
            for copy in upward:
                copy().start()

        @pl.when(has_down)
        def _():
            for copy in downward:
                copy().start()

    def start_diagonals(X, m):
        start_up_down([partial(diag_up, X, m, n) for n in range(2)], [partial(diag_down, X, m, n) for n in range(2)])

    def wait_rows(upward, downward):
        @pl.when(has_down)
        def _():
            upward().wait_recv()
            downward().wait_send()

        @pl.when(has_up)
        def _():
            downward().wait_recv()
            upward().wait_send()

    loads[0].wait()
    loads[1].wait()
    for i in range(2):
        for r in range(rows):
            w = winds[pl.ds(i * levels * rows + r, levels, stride=rows), :] * 0.5
            d = diff[pl.ds(r, 1), :]
            PK[i, r + 1, own, :] = jnp.concatenate([w + d, w - d], axis=0).T

    @pl.loop(0, groups)
    def _(g):
        state_load(g).wait()
        for r in range(rows):
            H[0, g, r + 1, own, :] = state[pl.ds(g * LANES * rows + r, LANES, stride=rows), :].T

    edge = jnp.zeros((span, LANES), jnp.float32)

    @pl.when(jnp.logical_not(has_up))
    def _():
        PK[1, 0, wide, :] = edge

        @pl.loop(0, total * groups)
        def _(n):
            for X in (H, Y):
                X[n // groups, n % groups, above, wide, :] = edge

    @pl.when(jnp.logical_not(has_down))
    def _():
        @pl.loop(0, total * groups)
        def _(n):
            for X in (H, Y):
                X[n // groups, n % groups, below, wide, :] = edge

    pl.semaphore_wait(barrier, devices - 1)

    for copy in pk_lon():
        copy.start()
    start_up_down((), [partial(pk_down, n) for n in range(3)])
    for copy in lon_halo(H, 0, 0):
        copy.start()
    start_diagonals(H, 0)

    @pl.loop(0, groups)
    def _(g):
        start_up_down([lambda: row_up(H, 0, g)], [lambda: row_down(H, 0, g)])

    for load in loads[3:]:
        load.start()
    loads[2].wait()

    @pl.loop(0, slots)
    def _(k):
        for c in range(capacity):
            for h in range(chunks):
                SB[k, pl.ds(c * chunks + h, devices, stride=block), :] = obs[k, c, :, pl.ds(h * LANES, LANES)]
        for c in range(capacity * chunks, block):
            SB[k, pl.ds(c, devices, stride=block), :] = jnp.zeros((devices, LANES), jnp.float32)
        GOT[k, pl.ds(me * block, block), :] = SB[k, pl.ds(me * block, block), :]

    @pl.loop(0, slots * (devices - 1))
    def _(n):
        hand_over(n // (devices - 1), n % (devices - 1)).start()

    loads[3].wait()
    loads[4].wait()
    part = channels // 7

    @pl.loop(0, 14)
    def _(n):
        at = pl.ds(n % 7 * part, part)
        high, low = split2(tables[n // 7, at, :])
        TB[n // 7, at, pl.ds(0, prof)] = high
        TB[n // 7, at, pl.ds(prof, prof)] = low

    for copy in pk_lon():
        copy.wait_recv()

    @pl.when(has_up)
    def _():
        for n in range(3):
            pk_down(n).wait_recv()

    lower = lax.broadcasted_iota(jnp.int32, (span, LANES), 1) < levels

    def unpack(v):
        other = pltpu.roll(v, levels, 1)
        return jnp.where(lower, v, other), jnp.where(lower, other, v)

    def fill(C, r, signs):
        a, b = unpack(PK[0, r + 1, wide, :])
        aw, bw = unpack(PK[0, r + 1, pl.ds(PAD - EXT - 1, span), :])
        al, bl = unpack(PK[1, r + 1, wide, :])
        au, bu = unpack(PK[1, r, wide, :])
        C[0, r] = 1.0 - a + bw - al + bu
        for n, v in enumerate((-b, aw, -bl, au) if signs else (a, -bw, al, -bu)):
            C[n + 1, r] = v

    @pl.loop(0, rows)
    def _(r):
        fill(F, r, True)

    first_count = steps_ref[0]
    second_count = steps_ref[1]
    kept = min(MAXSTEP, total - 1)

    def advance(X, C, s, g, which, flag=None):
        for c in range(0, span, COLS):
            at = pl.ds(PAD - EXT + c, COLS)
            cat = pl.ds(c, COLS)
            row = {n: X[s, g, n, at, :] for n in sorted({r + d for r in which for d in range(3)})}
            for r in which:
                new = C[0, r, cat, :] * row[r + 1]
                new = new + C[3, r, cat, :] * row[r + 2]
                new = new + C[4, r, cat, :] * row[r]
                new = new + C[1, r, cat, :] * X[s, g, r + 1, pl.ds(PAD - EXT + c + 1, COLS), :]
                new = new + C[2, r, cat, :] * X[s, g, r + 1, pl.ds(PAD - EXT + c - 1, COLS), :]
                if flag is not None:
                    new = new + jnp.where(flag, Y[total + 1, g, r + 1, at, :], 0.0)
                X[s + 1, g, r + 1, at, :] = new

    def turn(X, C, m, s, g, flag=None):
        @pl.when(s == 0)
        def _():
            wait_rows(lambda: row_up(X, m, g), lambda: row_down(X, m, g))

        @pl.when(s > 0)
        def _():
            wait_rows(lambda: lat_up(X, m, s, g), lambda: lat_down(X, m, s, g))

        advance(X, C, s, g, (0, rows - 1), flag)

        @pl.when(s < total - 1)
        def _():
            start_up_down([lambda: lat_up(X, m, s + 1, g)], [lambda: lat_down(X, m, s + 1, g)])

        advance(X, C, s, g, tuple(range(1, rows - 1)), flag)

        if flag is None:
            @pl.when(s < kept)
            def _():
                for r in range(rows):
                    H[total + 1, g, r + 1, own, :] = jnp.where(
                        s < first_count, H[s + 1, g, r + 1, own, :], H[total + 1, g, r + 1, own, :])

    def wait_edges(X, n, m, diagonals=True):
        for copy in lon_halo(X, n, m):
            copy.wait()
        if diagonals:
            @pl.when(has_down)
            def _():
                for n in range(2):
                    diag_up(X, m, n).wait_recv()
                    diag_down(X, m, n).wait_send()

            @pl.when(has_up)
            def _():
                for n in range(2):
                    diag_down(X, m, n).wait_recv()
                    diag_up(X, m, n).wait_send()

    def select(n):
        b = n % chunks
        column = jnp.broadcast_to(chan_ref[pl.ds(b, 1), :].astype(jnp.float32), (LANES, LANES)).T
        column = jnp.concatenate([column] * -(-channels // LANES), axis=1)[:, :channels]
        picker = (column == lax.broadcasted_iota(jnp.int32, (LANES, channels), 1).astype(jnp.float32)).astype(
            jnp.float32).astype(jnp.bfloat16)
        AE[pl.ds(n * LANES, LANES), :] = dot(picker, TB[n // chunks]).astype(jnp.bfloat16)

        @pl.when(n < chunks)
        def _():
            weights = jnp.concatenate(
                [jnp.broadcast_to(v, (8, channels)) for v in split3(weight_ref[...].reshape(1, channels))], axis=0)
            w = dot(weights, picker, LAST)
            WS[pl.ds(b, 1), :] = w[0:1] + w[8:9] + w[16:17]

    earlier = lax.broadcasted_iota(jnp.int32, (soundings, soundings), 0) < lax.broadcasted_iota(
        jnp.int32, (soundings, soundings), 1)

    def collect(k):
        @pl.loop(0, devices - 1)
        def _(n):
            hand_over(k, n).wait_recv()

        owner = owner_ref[k]
        spread = jnp.broadcast_to(owner.astype(jnp.float32), (soundings, soundings))
        same = jnp.logical_and(spread.T == spread, earlier)
        rank = jnp.sum(same.astype(jnp.float32), axis=0, keepdims=True).astype(jnp.int32)
        places = block // chunks
        source = one_hot(owner * places + rank, devices * places)
        for h in range(chunks):
            got = dot(source, jnp.concatenate(split2(GOT[k, pl.ds(h, devices * places, stride=chunks), :]), axis=1), FIRST)
            WN[k, :, pl.ds(h * LANES, LANES)] = got[:, :LANES] + got[:, LANES:]

    def observe(k):
        placed = one_hot(cell_ref[pl.ds(k, 1), :], cells)
        weight = jnp.concatenate([WS[b:b + 1, :] for b in range(chunks)], axis=1)
        high, low = [], []
        for g in range(groups):
            field = H[total + 1 - k, g, inner, own, :].reshape(cells, LANES)
            taken = dot(placed, jnp.concatenate(split2(field), axis=1), FIRST).astype(jnp.bfloat16)
            high.append(taken[:, :LANES])
            low.append(taken[:, LANES:])
        high = jnp.concatenate(high, axis=1)
        low = jnp.concatenate(low, axis=1)
        table, rest = AE[:, pl.ds(0, prof)], AE[:, pl.ds(prof, prof)]
        both = dot(jnp.concatenate([high, low], axis=0), table, LAST)
        both = both[:soundings] + both[soundings:] + dot(high, rest, LAST)
        optical, bright = both[:, :used], both[:, used:]
        small = jnp.exp(-jnp.abs(optical))
        inv = 1.0 / (1.0 + small)
        passed = jnp.where(optical > 0, small, 1.0) * inv
        slope = jnp.where(optical > 0, 1.0, small) * inv
        y = passed * bright
        departure = weight * (y - WN[k])
        high, low = split2(jnp.concatenate([-(departure * y) * slope, departure * passed], axis=1))
        both = dot(jnp.concatenate([high, low], axis=0), table)
        back = both[:soundings] + both[soundings:] + dot(high, rest)
        back = jnp.concatenate(split2(back), axis=0)
        placed = jnp.concatenate([placed, placed], axis=1)
        target = jnp.where(k == 0, total + 1, 0)
        for g in range(groups):
            Y[target, g, inner, own, :] = dot(placed, back[:, g * LANES:(g + 1) * LANES]).reshape(rows, width, LANES)

        for copy in lon_halo(Y, target, 2 - k):
            copy.start()

        @pl.when(k > 0)
        def _():
            start_diagonals(Y, 1)

            @pl.loop(0, groups)
            def _(g):
                start_up_down([lambda: row_up(Y, 1, g)], [lambda: row_down(Y, 1, g)])

    wait_edges(H, 0, 0)
    turns = total * groups
    early = kept * groups - 1
    ready = turns if total < 4 else turns - 2

    @pl.loop(0, turns + 1)
    def _(it):
        @pl.when(it < turns)
        def _():
            turn(H, F, 0, it // groups, it % groups)

        @pl.when(jnp.logical_and(it > 0, it <= rows))
        def _():
            fill(B, it - 1, False)

        for n in range(-(-2 * chunks // (kept * groups))):
            at = it + n * kept * groups

            @pl.when(jnp.logical_and(it < kept * groups, at < 2 * chunks))
            def _():
                select(at)

        @pl.when(jnp.logical_or(it == early, it == ready))
        def _():
            collect((it == ready).astype(jnp.int32))

        @pl.when(jnp.logical_or(it == early, it == turns))
        def _():
            observe((it == turns).astype(jnp.int32))

    @pl.loop(0, slots * (devices - 1))
    def _(n):
        hand_over(n // (devices - 1), n % (devices - 1)).wait_send()

    for copy in pk_lon():
        copy.wait_send()

    @pl.when(has_down)
    def _():
        for n in range(3):
            pk_down(n).wait_send()

    wait_edges(Y, 0, 1)
    wait_edges(Y, total + 1, 2, diagonals=False)

    @pl.loop(0, turns)
    def _(it):
        s = it // groups
        g = it % groups
        turn(Y, B, 1, s, g, s + 1 == second_count)

        @pl.when(s == total - 1)
        def _():
            for r in range(rows):
                out_ref[pl.ds(g * LANES * rows + r, LANES, stride=rows), :] = Y[total, g, r + 1, own, :].T


def whole_call(lat_count, lon_count, total, step_counts, state, winds, diffusivity, by_rank, absorb, emit,
               cells, owners, channel_list, weight):
    rows, width = diffusivity.shape
    groups = state.shape[0] // (rows * LANES)
    slots, capacity, devices, used = by_rank.shape
    channels, prof = absorb.shape
    block = -(-capacity * (used // LANES) // 8) * 8
    wide = width + 2 * PAD
    span = width + 2 * EXT
    vmem = pl.BlockSpec(memory_space=pltpu.VMEM)
    hbm = pl.BlockSpec(memory_space=pl.ANY)
    f32, bf16 = jnp.float32, jnp.bfloat16
    dma = pltpu.SemaphoreType.DMA
    scratch = [
        pltpu.VMEM(state.shape, f32), pltpu.VMEM(winds.shape, f32), pltpu.VMEM(diffusivity.shape, f32),
        pltpu.VMEM(by_rank.shape, f32), pltpu.VMEM((2, channels, prof), f32),
        pltpu.VMEM((2, channels, 2 * prof), bf16), pltpu.VMEM((2 * used, 2 * prof), bf16),
        pltpu.VMEM((used // LANES, LANES), f32),
        pltpu.VMEM((total + 2, groups, rows + 2, wide, LANES), f32),
        pltpu.VMEM((total + 2, groups, rows + 2, wide, LANES), f32),
        pltpu.VMEM((5, rows, span, LANES), f32), pltpu.VMEM((5, rows, span, LANES), f32),
        pltpu.VMEM((2, rows + 1, wide, LANES), f32),
        pltpu.VMEM((slots, devices * block, LANES), f32), pltpu.VMEM((slots, devices * block, LANES), f32),
        pltpu.VMEM((slots, cells.shape[1], used), f32),
        dma((5,)), dma((groups,)), dma((5,)), dma((5,)), dma((2, groups, 2)), dma((2, groups, 2)), dma((3, 2)), dma((3, 2)),
        dma((2, 4)), dma((2, 4)), dma((2, total, groups, 2)), dma((2, total, groups, 2)),
        dma((slots, devices)), dma((slots, devices)),
    ]
    return pl.pallas_call(
        partial(whole_kernel, total, lat_count, lon_count),
        out_shape=jax.ShapeDtypeStruct(state.shape, f32),
        in_specs=[pl.BlockSpec(memory_space=pltpu.SMEM)] + [hbm] * 6 + [vmem] * 4,
        out_specs=vmem,
        scratch_shapes=scratch,
        compiler_params=pltpu.CompilerParams(
            collective_id=total, has_side_effects=True, vmem_limit_bytes=60 << 20),
        name="whole",
    )(step_counts, state, winds, diffusivity, by_rank, absorb, emit, cells, owners, channel_list, weight)


def form_kernel(slots, steps_ref, out_ref):
    out_ref[0] = steps_ref[0] + steps_ref[1] - slots


def form_of(step_counts, slots):
    smem = pl.BlockSpec(memory_space=pltpu.SMEM)
    return pl.pallas_call(partial(form_kernel, slots), out_shape=jax.ShapeDtypeStruct((1,), jnp.int32),
                          in_specs=[smem], out_specs=smem, name="form")(step_counts)


def per_device(lat_count, lon_count, state, winds, diffusivity, sounding_cell, sounding_owner,
               step_counts, channel_list, absorb_table, emit_table, obs_weight, observed):
    width = state.shape[-1]
    operands = (
        step_counts, state.reshape(-1, width), winds.reshape(-1, width), diffusivity,
        jnp.transpose(observed[:, 0], (0, 2, 1, 3)), absorb_table.T, emit_table.T,
        sounding_cell, jnp.transpose(sounding_owner, (0, 2, 1)), channel_list.reshape(-1, LANES),
        obs_weight)
    slots = step_counts.shape[0]
    branches = [partial(whole_call, lat_count, lon_count, n) for n in range(slots, slots * MAXSTEP + 1)]
    return lax.switch(form_of(step_counts, slots)[0], branches, *operands).reshape(state.shape)


def solution(mesh):
    return jax.shard_map(
        partial(per_device, mesh.shape["lat"], mesh.shape["lon"]),
        mesh=mesh,
        in_specs=(
            P(None, None, "lat", "lon"),
            P(None, None, "lat", "lon"),
            P("lat", "lon"),
            P(None, ("lon", "lat")),
            P(None, ("lon", "lat"), None),
            P(),
            P(),
            P(),
            P(),
            P(),
            P(None, ("lon", "lat"), None, None, None),
        ),
        out_specs=P(None, None, "lat", "lon"),
        check_vma=False,
    )
```

```python
from functools import partial

import jax
import jax.numpy as jnp
from jax import lax
from jax.experimental import pallas as pl
from jax.experimental.pallas import tpu as pltpu
from jax.sharding import PartitionSpec as P

MAXSTEP = 4
LANES = 128
EXT = 8
PAD = 16
COLS = 24
RING = 4
MESH_ID = pl.DeviceIdType.MESH
FIRST = ((0,), (0,))
LAST = ((1,), (1,))


def split2(v):
    high = v.astype(jnp.bfloat16)
    return high, (v - high.astype(jnp.float32)).astype(jnp.bfloat16)


def split3(v):
    high = v.astype(jnp.bfloat16)
    rest = v - high.astype(jnp.float32)
    mid = rest.astype(jnp.bfloat16)
    return high, mid, (rest - mid.astype(jnp.float32)).astype(jnp.bfloat16)


def dot(a, b, dims=((1,), (0,))):
    return lax.dot_general(a, b, (dims, ((), ())), preferred_element_type=jnp.float32)


def one_hot(row, size):
    return (row == lax.broadcasted_iota(jnp.int32, (size, row.shape[1]), 0)).astype(
        jnp.float32).astype(jnp.bfloat16)


def whole_kernel(total, lat_count, lon_count, *refs):
    (steps_ref, state_hbm, winds_hbm, diff_hbm, obs_hbm, absorb_hbm, emit_hbm, cell_ref, owner_ref, chan_ref,
     weight_ref, out_ref,
     state, winds, diff, obs, tables, TB, AE, WS, H, Y, F, B, PK, SB, GOT, WN,
     local_sem, state_sem, pk_s, pk_r, row_s, row_r, lon_s, lon_r, diag_s, diag_r, lat_s, lat_r, obs_s, obs_r) = refs
    groups, rows = H.shape[1], H.shape[2] - 4
    width = state.shape[1]
    span = width + 2 * EXT
    levels = winds.shape[0] // (2 * rows)
    devices = lat_count * lon_count
    slots, capacity, _, used = obs.shape
    chunks = used // LANES
    block = SB.shape[1] // devices
    channels, prof = tables.shape[1:]
    cells = rows * width
    soundings = cell_ref.shape[1]
    lat = lax.axis_index("lat")
    lon = lax.axis_index("lon")
    me = lon * lat_count + lat
    east = lax.rem(lon + 1, lon_count)
    west = lax.rem(lon + lon_count - 1, lon_count)
    has_up = lat > 0
    has_down = lat < lat_count - 1
    up, down = lat - 1, lat + 1
    own = pl.ds(PAD, width)
    wide = pl.ds(PAD - EXT, span)
    head, tail = pl.ds(PAD, EXT), pl.ds(PAD + width - EXT, EXT)
    before, after = pl.ds(PAD - EXT, EXT), pl.ds(PAD + width, EXT)
    inner = pl.ds(2, rows)
    top, bottom, above, below = 2, rows + 1, 1, rows + 2

    loads = [pltpu.make_async_copy(src, dst, local_sem.at[n]) for n, (src, dst) in enumerate((
        (winds_hbm, winds), (diff_hbm, diff), (obs_hbm, obs),
        (absorb_hbm, tables.at[0]), (emit_hbm, tables.at[1])))]
    for load in loads[:2]:
        load.start()

    def state_load(g):
        at = pl.ds(g * LANES * rows, LANES * rows)
        return pltpu.make_async_copy(state_hbm.at[at], state.at[at], state_sem.at[g])

    @pl.loop(0, groups)
    def _(g):
        state_load(g).start()

    loads[2].start()
    barrier = pltpu.get_barrier_semaphore()

    @pl.loop(1, devices)
    def _(j):
        other = (me + j) % devices
        pl.semaphore_signal(barrier, inc=1, device_id={"lon": other // lat_count, "lat": other % lat_count},
                            device_id_type=MESH_ID)

    def remote(src, dst, s, r, to_lat, to_lon):
        return pltpu.make_async_remote_copy(
            src, dst, s, r, device_id={"lon": to_lon, "lat": to_lat}, device_id_type=MESH_ID)

    middle = lon_count // 2 * lat_count

    def hand_over(k, n):
        shift = n + n // middle
        to_lon = lax.rem(lon + lon_count // 2 + shift // lat_count, lon_count)
        to_lat = lax.rem(lat + shift % lat_count, lat_count)
        other = to_lon * lat_count + to_lat
        return remote(SB.at[k, pl.ds(other * block, block)], GOT.at[k, pl.ds(me * block, block)],
                      obs_s.at[k, n], obs_r.at[k, n], to_lat, to_lon)

    def pk_lon():
        return (remote(PK.at[:, inner, tail], PK.at[:, inner, before], pk_s.at[0], pk_r.at[0], lat, east),
                remote(PK.at[:, inner, head], PK.at[:, inner, after], pk_s.at[1], pk_r.at[1], lat, west))

    def pk_piece(n, where):
        src, dst, to_lon = ((own, own, lon), (tail, before, east), (head, after, west))[n]
        srcs, dsts, to_lat, m = {
            "near": (PK.at[1, bottom, src], PK.at[1, above, dst], down, 2),
            "far": (PK.at[1, bottom - 1, src], PK.at[1, above - 1, dst], down, 5),
            "side": (PK.at[0, bottom, src], PK.at[0, above, dst], down, 8),
            "up": (PK.at[:, top, src], PK.at[:, below, dst], up, 11)}[where]
        return remote(srcs, dsts, pk_s.at[m + n], pk_r.at[m + n], to_lat, to_lon)

    def lon_halo(X, n, m):
        return (remote(X.at[n, :, inner, tail], X.at[n, :, inner, before], lon_s.at[m, 0], lon_r.at[m, 0], lat, east),
                remote(X.at[n, :, inner, head], X.at[n, :, inner, after], lon_s.at[m, 1], lon_r.at[m, 1], lat, west))

    def diag_up(X, at, m, n):
        src, dst, to_lon = ((tail, before, east), (head, after, west))[n]
        return remote(X.at[at, :, pl.ds(top, 2), src], X.at[at, :, pl.ds(below, 2), dst],
                      diag_s.at[m, n], diag_r.at[m, n], up, to_lon)

    def diag_down(X, at, m, n):
        src, dst, to_lon = ((tail, before, east), (head, after, west))[n]
        return remote(X.at[at, :, pl.ds(bottom - 1, 2), src], X.at[at, :, pl.ds(above - 1, 2), dst],
                      diag_s.at[m, 2 + n], diag_r.at[m, 2 + n], down, to_lon)

    def row_up(X, at, m, g, d):
        return remote(X.at[at, g, top + d, own], X.at[at, g, below + d, own],
                      row_s.at[m, g, d, 0], row_r.at[m, g, d, 0], up, lon)

    def row_down(X, at, m, g, d):
        return remote(X.at[at, g, bottom - d, own], X.at[at, g, above - d, own],
                      row_s.at[m, g, d, 1], row_r.at[m, g, d, 1], down, lon)

    margin = max(total - 3, 0)
    some = pl.ds(PAD - margin, width + 2 * margin)

    def lat_up(X, m, s, g):
        n = s % RING
        return remote(X.at[n, g, top + 1, some], X.at[n, g, below + 1, some],
                      lat_s.at[m, s, g, 0], lat_r.at[m, s, g, 0], up, lon)

    def lat_down(X, m, s, g):
        n = s % RING
        return remote(X.at[n, g, bottom - 1, some], X.at[n, g, above - 1, some],
                      lat_s.at[m, s, g, 1], lat_r.at[m, s, g, 1], down, lon)

    def start_up_down(upward, downward):
        @pl.when(has_up)
        def _():
            for copy in upward:
                copy().start()

        @pl.when(has_down)
        def _():
            for copy in downward:
                copy().start()

    def start_diagonals(X, at, m):
        start_up_down([partial(diag_up, X, at, m, n) for n in range(2)],
                      [partial(diag_down, X, at, m, n) for n in range(2)])

    def start_rows(X, at, m, d):
        @pl.loop(0, groups)
        def _(g):
            start_up_down([lambda: row_up(X, at, m, g, d)], [lambda: row_down(X, at, m, g, d)])

    def wait_rows(upward, downward):
        @pl.when(has_down)
        def _():
            upward().wait_recv()
            downward().wait_send()

        @pl.when(has_up)
        def _():
            downward().wait_recv()
            upward().wait_send()

    loads[0].wait()
    loads[1].wait()
    for i in range(2):
        for r in range(rows):
            w = winds[pl.ds(i * levels * rows + r, levels, stride=rows), :] * 0.5
            d = diff[pl.ds(r, 1), :]
            PK[i, r + 2, own, :] = jnp.concatenate([w + d, w - d], axis=0).T

    @pl.loop(0, groups)
    def _(g):
        state_load(g).wait()
        for r in range(rows):
            H[0, g, r + 2, own, :] = state[pl.ds(g * LANES * rows + r, LANES, stride=rows), :].T

    edge = jnp.zeros((span, LANES), jnp.float32)

    @pl.when(jnp.logical_not(has_up))
    def _():
        PK[1, above, wide, :] = edge

    pl.semaphore_wait(barrier, devices - 1)

    for copy in pk_lon():
        copy.start()
    start_up_down((), [partial(pk_piece, n, "near") for n in range(3)])
    for copy in lon_halo(H, 0, 0):
        copy.start()
    start_diagonals(H, 0, 0)
    start_rows(H, 0, 0, 0)
    start_up_down([partial(pk_piece, n, "up") for n in range(3)],
                  [partial(pk_piece, n, w) for w in ("side", "far") for n in range(3)])
    start_rows(H, 0, 0, 1)

    for load in loads[3:]:
        load.start()
    loads[2].wait()

    @pl.loop(0, slots)
    def _(k):
        for c in range(capacity):
            for h in range(chunks):
                SB[k, pl.ds(c * chunks + h, devices, stride=block), :] = obs[k, c, :, pl.ds(h * LANES, LANES)]
        for c in range(capacity * chunks, block):
            SB[k, pl.ds(c, devices, stride=block), :] = jnp.zeros((devices, LANES), jnp.float32)
        GOT[k, pl.ds(me * block, block), :] = SB[k, pl.ds(me * block, block), :]

    @pl.loop(0, slots * (devices - 1))
    def _(n):
        hand_over(n // (devices - 1), n % (devices - 1)).start()

    def clear(first):
        @pl.loop(0, (RING + 1) * groups)
        def _(n):
            for X in (H, Y):
                for r in (first, first + 1):
                    X[n // groups, n % groups, r, wide, :] = edge

    @pl.when(jnp.logical_not(has_up))
    def _():
        clear(0)

    @pl.when(jnp.logical_not(has_down))
    def _():
        clear(below)

    loads[3].wait()
    loads[4].wait()
    part = channels // 7

    @pl.loop(0, 14)
    def _(n):
        at = pl.ds(n % 7 * part, part)
        high, low = split2(tables[n // 7, at, :])
        TB[n // 7, at, pl.ds(0, prof)] = high
        TB[n // 7, at, pl.ds(prof, prof)] = low

    for copy in pk_lon():
        copy.wait_recv()

    @pl.when(has_up)
    def _():
        for n in range(3):
            pk_piece(n, "near").wait_recv()

    lower = lax.broadcasted_iota(jnp.int32, (span, LANES), 1) < levels

    def unpack(v):
        other = pltpu.roll(v, levels, 1)
        return jnp.where(lower, v, other), jnp.where(lower, other, v)

    def fill(C, q, signs):
        a, b = unpack(PK[0, q + 1, wide, :])
        aw, bw = unpack(PK[0, q + 1, pl.ds(PAD - EXT - 1, span), :])
        al, bl = unpack(PK[1, q + 1, wide, :])
        au, bu = unpack(PK[1, q, wide, :])
        real = jnp.logical_and(jnp.logical_or(q > 0, has_up), jnp.logical_or(q <= rows, has_down))
        values = (-b, aw, -bl, au) if signs else (a, -bw, al, -bu)
        for n, v in enumerate((1.0 - a + bw - al + bu,) + values):
            C[n, q] = jnp.where(real, v, 0.0)

    @pl.loop(1, rows + 1)
    def _(q):
        fill(F, q, True)

    first_count = steps_ref[0]
    second_count = steps_ref[1]
    kept = min(MAXSTEP, total - 1)

    def advance(X, C, src, dst, g, which, flag):
        for c in range(0, span, COLS):
            at = pl.ds(PAD - EXT + c, COLS)
            cat = pl.ds(c, COLS)
            row = {n: X[src, g, n, at, :] for n in sorted({r + d for r in which for d in (-1, 0, 1)})}
            for r in which:
                new = C[0, r - 1, cat, :] * row[r]
                new = new + C[3, r - 1, cat, :] * row[r + 1]
                new = new + C[4, r - 1, cat, :] * row[r - 1]
                new = new + C[1, r - 1, cat, :] * X[src, g, r, pl.ds(PAD - EXT + c + 1, COLS), :]
                new = new + C[2, r - 1, cat, :] * X[src, g, r, pl.ds(PAD - EXT + c - 1, COLS), :]
                if flag is not None:
                    new = new + jnp.where(flag, Y[RING, g, r, at, :], 0.0)
                X[dst, g, r, at, :] = new

    sent = tuple(sorted({top + 1, bottom - 1}))
    kept_rows = tuple(r for r in range(top, bottom + 1) if r not in sent)

    def turn(X, C, m, s, g, count=None):
        here, there = s % RING, (s + 1) % RING
        flag = None if count is None else s + 1 == count

        @pl.when(s == 0)
        def _():
            wait_rows(lambda: row_up(X, 0, m, g, 0), lambda: row_down(X, 0, m, g, 0))

        @pl.when(s == 1)
        def _():
            wait_rows(lambda: row_up(X, 0, m, g, 1), lambda: row_down(X, 0, m, g, 1))

        @pl.when(s > 1)
        def _():
            wait_rows(lambda: lat_up(X, m, s - 1, g), lambda: lat_down(X, m, s - 1, g))

        @pl.when(s > 0)
        def _():
            advance(X, C, (s + RING - 1) % RING, here, g, (above, below), None if count is None else s == count)

        advance(X, C, here, there, g, sent, flag)

        @pl.when(s < total - 2)
        def _():
            start_up_down([lambda: lat_up(X, m, s + 1, g)], [lambda: lat_down(X, m, s + 1, g)])

        advance(X, C, here, there, g, kept_rows, flag)

        if count is None:
            @pl.when(s < kept)
            def _():
                for r in range(top, bottom + 1):
                    H[RING, g, r, own, :] = jnp.where(s < first_count, H[there, g, r, own, :], H[RING, g, r, own, :])

    def wait_edges(X, at, m):
        for copy in lon_halo(X, at, m):
            copy.wait()

        @pl.when(has_down)
        def _():
            for n in range(2):
                diag_up(X, at, m, n).wait_recv()
                diag_down(X, at, m, n).wait_send()

        @pl.when(has_up)
        def _():
            for n in range(2):
                diag_down(X, at, m, n).wait_recv()
                diag_up(X, at, m, n).wait_send()

    def select(n):
        b = n % chunks
        column = jnp.broadcast_to(chan_ref[pl.ds(b, 1), :].astype(jnp.float32), (LANES, LANES)).T
        column = jnp.concatenate([column] * -(-channels // LANES), axis=1)[:, :channels]
        picker = (column == lax.broadcasted_iota(jnp.int32, (LANES, channels), 1).astype(jnp.float32)).astype(
            jnp.float32).astype(jnp.bfloat16)
        AE[pl.ds(n * LANES, LANES), :] = dot(picker, TB[n // chunks]).astype(jnp.bfloat16)

        @pl.when(n < chunks)
        def _():
            weights = jnp.concatenate(
                [jnp.broadcast_to(v, (8, channels)) for v in split3(weight_ref[...].reshape(1, channels))], axis=0)
            w = dot(weights, picker, LAST)
            WS[pl.ds(b, 1), :] = w[0:1] + w[8:9] + w[16:17]

    earlier = lax.broadcasted_iota(jnp.int32, (soundings, soundings), 0) < lax.broadcasted_iota(
        jnp.int32, (soundings, soundings), 1)

    def collect(k):
        @pl.loop(0, devices - 1)
        def _(n):
            hand_over(k, n).wait_recv()

        owner = owner_ref[k]
        spread = jnp.broadcast_to(owner.astype(jnp.float32), (soundings, soundings))
        same = jnp.logical_and(spread.T == spread, earlier)
        rank = jnp.sum(same.astype(jnp.float32), axis=0, keepdims=True).astype(jnp.int32)
        places = block // chunks
        source = one_hot(owner * places + rank, devices * places)
        for h in range(chunks):
            got = dot(source, jnp.concatenate(split2(GOT[k, pl.ds(h, devices * places, stride=chunks), :]), axis=1), FIRST)
            WN[k, :, pl.ds(h * LANES, LANES)] = got[:, :LANES] + got[:, LANES:]

    def observe(k):
        placed = one_hot(cell_ref[pl.ds(k, 1), :], cells)
        weight = jnp.concatenate([WS[b:b + 1, :] for b in range(chunks)], axis=1)
        high, low = [], []
        for g in range(groups):
            field = H[jnp.where(k == 0, RING, total % RING), g, inner, own, :].reshape(cells, LANES)
            taken = dot(placed, jnp.concatenate(split2(field), axis=1), FIRST).astype(jnp.bfloat16)
            high.append(taken[:, :LANES])
            low.append(taken[:, LANES:])
        high = jnp.concatenate(high, axis=1)
        low = jnp.concatenate(low, axis=1)
        table, rest = AE[:, pl.ds(0, prof)], AE[:, pl.ds(prof, prof)]
        both = dot(jnp.concatenate([high, low], axis=0), table, LAST)
        both = both[:soundings] + both[soundings:] + dot(high, rest, LAST)
        optical, bright = both[:, :used], both[:, used:]
        small = jnp.exp(-jnp.abs(optical))
        inv = 1.0 / (1.0 + small)
        passed = jnp.where(optical > 0, small, 1.0) * inv
        slope = jnp.where(optical > 0, 1.0, small) * inv
        y = passed * bright
        departure = weight * (y - WN[k])
        high, low = split2(jnp.concatenate([-(departure * y) * slope, departure * passed], axis=1))
        both = dot(jnp.concatenate([high, low], axis=0), table)
        back = both[:soundings] + both[soundings:] + dot(high, rest)
        back = jnp.concatenate(split2(back), axis=0)
        placed = jnp.concatenate([placed, placed], axis=1)
        target = jnp.where(k == 0, RING, 0)
        for g in range(groups):
            Y[target, g, inner, own, :] = dot(placed, back[:, g * LANES:(g + 1) * LANES]).reshape(rows, width, LANES)

        for copy in lon_halo(Y, target, 2 - k):
            copy.start()

        start_diagonals(Y, target, 2 - k)
        start_rows(Y, target, 2 - k, 0)

        @pl.when(k > 0)
        def _():
            start_rows(Y, 0, 1, 1)

    wait_edges(H, 0, 0)
    turns = total * groups
    early = (total - 1) * groups - 1
    ready = turns if total < 4 else turns - 2

    @pl.loop(0, turns + 1)
    def _(it):
        @pl.when(it == groups)
        def _():
            @pl.when(has_down)
            def _():
                for n in range(3):
                    pk_piece(n, "up").wait_recv()
                    for w in ("near", "side", "far"):
                        pk_piece(n, w).wait_send()

            @pl.when(has_up)
            def _():
                for n in range(3):
                    pk_piece(n, "up").wait_send()
                    for w in ("side", "far"):
                        pk_piece(n, w).wait_recv()

            fill(F, 0, True)
            fill(F, rows + 1, True)

        @pl.when(it < turns)
        def _():
            turn(H, F, 0, it // groups, it % groups)

        @pl.when(it == groups + 1)
        def _():
            @pl.loop(0, rows + 2)
            def _(q):
                fill(B, q, False)

        for n in range(-(-2 * chunks // (kept * groups))):
            at = it + n * kept * groups

            @pl.when(jnp.logical_and(it < kept * groups, at < 2 * chunks))
            def _():
                select(at)

        @pl.when(jnp.logical_or(it == early, it == ready))
        def _():
            collect((it == ready).astype(jnp.int32))

        @pl.when(jnp.logical_or(it == early, it == turns))
        def _():
            observe((it == turns).astype(jnp.int32))

    @pl.loop(0, slots * (devices - 1))
    def _(n):
        hand_over(n // (devices - 1), n % (devices - 1)).wait_send()

    for copy in pk_lon():
        copy.wait_send()

    wait_edges(Y, 0, 1)
    wait_edges(Y, RING, 2)

    @pl.loop(0, groups)
    def _(g):
        wait_rows(lambda: row_up(Y, RING, 2, g, 0), lambda: row_down(Y, RING, 2, g, 0))

    @pl.loop(0, turns)
    def _(it):
        s = it // groups
        g = it % groups
        turn(Y, B, 1, s, g, second_count)

        @pl.when(s == total - 1)
        def _():
            for r in range(rows):
                out_ref[pl.ds(g * LANES * rows + r, LANES, stride=rows), :] = Y[total % RING, g, r + 2, own, :].T


def whole_call(lat_count, lon_count, total, step_counts, state, winds, diffusivity, by_rank, absorb, emit,
               cells, owners, channel_list, weight):
    rows, width = diffusivity.shape
    groups = state.shape[0] // (rows * LANES)
    slots, capacity, devices, used = by_rank.shape
    channels, prof = absorb.shape
    block = -(-capacity * (used // LANES) // 8) * 8
    wide = width + 2 * PAD
    span = width + 2 * EXT
    vmem = pl.BlockSpec(memory_space=pltpu.VMEM)
    hbm = pl.BlockSpec(memory_space=pl.ANY)
    f32, bf16 = jnp.float32, jnp.bfloat16
    dma = pltpu.SemaphoreType.DMA
    scratch = [
        pltpu.VMEM(state.shape, f32), pltpu.VMEM(winds.shape, f32), pltpu.VMEM(diffusivity.shape, f32),
        pltpu.VMEM(by_rank.shape, f32), pltpu.VMEM((2, channels, prof), f32),
        pltpu.VMEM((2, channels, 2 * prof), bf16), pltpu.VMEM((2 * used, 2 * prof), bf16),
        pltpu.VMEM((used // LANES, LANES), f32),
        pltpu.VMEM((RING + 1, groups, rows + 4, wide, LANES), f32),
        pltpu.VMEM((RING + 1, groups, rows + 4, wide, LANES), f32),
        pltpu.VMEM((5, rows + 2, span, LANES), f32), pltpu.VMEM((5, rows + 2, span, LANES), f32),
        pltpu.VMEM((2, rows + 4, wide, LANES), f32),
        pltpu.VMEM((slots, devices * block, LANES), f32), pltpu.VMEM((slots, devices * block, LANES), f32),
        pltpu.VMEM((slots, cells.shape[1], used), f32),
        dma((5,)), dma((groups,)), dma((14,)), dma((14,)), dma((3, groups, 2, 2)), dma((3, groups, 2, 2)),
        dma((3, 2)), dma((3, 2)), dma((3, 4)), dma((3, 4)), dma((2, total, groups, 2)), dma((2, total, groups, 2)),
        dma((slots, devices)), dma((slots, devices)),
    ]
    return pl.pallas_call(
        partial(whole_kernel, total, lat_count, lon_count),
        out_shape=jax.ShapeDtypeStruct(state.shape, f32),
        in_specs=[pl.BlockSpec(memory_space=pltpu.SMEM)] + [hbm] * 6 + [vmem] * 4,
        out_specs=vmem,
        scratch_shapes=scratch,
        compiler_params=pltpu.CompilerParams(
            collective_id=total, has_side_effects=True, vmem_limit_bytes=60 << 20),
        name="whole",
    )(step_counts, state, winds, diffusivity, by_rank, absorb, emit, cells, owners, channel_list, weight)


def form_kernel(slots, steps_ref, out_ref):
    out_ref[0] = steps_ref[0] + steps_ref[1] - slots


def form_of(step_counts, slots):
    smem = pl.BlockSpec(memory_space=pltpu.SMEM)
    return pl.pallas_call(partial(form_kernel, slots), out_shape=jax.ShapeDtypeStruct((1,), jnp.int32),
                          in_specs=[smem], out_specs=smem, name="form")(step_counts)


def per_device(lat_count, lon_count, state, winds, diffusivity, sounding_cell, sounding_owner,
               step_counts, channel_list, absorb_table, emit_table, obs_weight, observed):
    width = state.shape[-1]
    operands = (
        step_counts, state.reshape(-1, width), winds.reshape(-1, width), diffusivity,
        jnp.transpose(observed[:, 0], (0, 2, 1, 3)), absorb_table.T, emit_table.T,
        sounding_cell, jnp.transpose(sounding_owner, (0, 2, 1)), channel_list.reshape(-1, LANES),
        obs_weight)
    slots = step_counts.shape[0]
    branches = [partial(whole_call, lat_count, lon_count, n) for n in range(slots, slots * MAXSTEP + 1)]
    return lax.switch(form_of(step_counts, slots)[0], branches, *operands).reshape(state.shape)


def solution(mesh):
    return jax.shard_map(
        partial(per_device, mesh.shape["lat"], mesh.shape["lon"]),
        mesh=mesh,
        in_specs=(
            P(None, None, "lat", "lon"),
            P(None, None, "lat", "lon"),
            P("lat", "lon"),
            P(None, ("lon", "lat")),
            P(None, ("lon", "lat"), None),
            P(),
            P(),
            P(),
            P(),
            P(),
            P(None, ("lon", "lat"), None, None, None),
        ),
        out_specs=P(None, None, "lat", "lon"),
        check_vma=False,
    )
```

```python
from functools import partial

import jax
import jax.numpy as jnp
from jax import lax
from jax.experimental import pallas as pl
from jax.experimental.pallas import tpu as pltpu
from jax.sharding import PartitionSpec as P

MAXSTEP = 4
LANES = 128
EXT = 8
PAD = 16
COLS = 24
RING = 4
MESH_ID = pl.DeviceIdType.MESH
FIRST = ((0,), (0,))
LAST = ((1,), (1,))


def split2(v):
    high = v.astype(jnp.bfloat16)
    return high, (v - high.astype(jnp.float32)).astype(jnp.bfloat16)


def split3(v):
    high = v.astype(jnp.bfloat16)
    rest = v - high.astype(jnp.float32)
    mid = rest.astype(jnp.bfloat16)
    return high, mid, (rest - mid.astype(jnp.float32)).astype(jnp.bfloat16)


def dot(a, b, dims=((1,), (0,))):
    return lax.dot_general(a, b, (dims, ((), ())), preferred_element_type=jnp.float32)


def one_hot(row, size):
    return (row == lax.broadcasted_iota(jnp.int32, (size, row.shape[1]), 0)).astype(
        jnp.float32).astype(jnp.bfloat16)


def whole_kernel(total, lat_count, lon_count, *refs):
    (steps_ref, state_hbm, winds_hbm, diff_hbm, obs_hbm, absorb_hbm, emit_hbm, cell_ref, owner_ref, chan_ref,
     weight_ref, out_ref,
     state, winds, diff, obs, tables, TB, AE, WS, H, Y, F, B, PK, SB, GOT, WN,
     local_sem, state_sem, pk_s, pk_r, row_s, row_r, lon_s, lon_r, diag_s, diag_r, lat_s, lat_r, obs_s, obs_r) = refs
    groups, rows = H.shape[1], diff.shape[0]
    width = state.shape[1]
    span = width + 2 * EXT
    levels = winds.shape[0] // (2 * rows)
    devices = lat_count * lon_count
    slots, capacity, _, used = obs.shape
    chunks = used // LANES
    block = SB.shape[1] // devices
    channels, prof = tables.shape[1:]
    cells = rows * width
    soundings = cell_ref.shape[1]
    lat = lax.axis_index("lat")
    lon = lax.axis_index("lon")
    me = lon * lat_count + lat
    east = lax.rem(lon + 1, lon_count)
    west = lax.rem(lon + lon_count - 1, lon_count)
    has_up = lat > 0
    has_down = lat < lat_count - 1
    up, down = lat - 1, lat + 1
    own = pl.ds(PAD, width)
    wide = pl.ds(PAD - EXT, span)
    head, tail = pl.ds(PAD, EXT), pl.ds(PAD + width - EXT, EXT)
    before, after = pl.ds(PAD - EXT, EXT), pl.ds(PAD + width, EXT)
    lead = total - 2 >= MAXSTEP
    ahead = 1 if lead else 0

    top, bottom, above, below = 1 + ahead, rows + ahead, ahead, rows + 1 + ahead
    inner = pl.ds(top, rows)

    def slot(n):
        return n if total < RING else lax.rem(n, RING)

    loads = [pltpu.make_async_copy(src, dst, local_sem.at[n]) for n, (src, dst) in enumerate((
        (winds_hbm, winds), (diff_hbm, diff), (obs_hbm, obs),
        (absorb_hbm, tables.at[0]), (emit_hbm, tables.at[1])))]
    for load in loads[:2]:
        load.start()

    def state_load(g):
        at = pl.ds(g * LANES * rows, LANES * rows)
        return pltpu.make_async_copy(state_hbm.at[at], state.at[at], state_sem.at[g])

    @pl.loop(0, groups)
    def _(g):
        state_load(g).start()

    loads[2].start()
    barrier = pltpu.get_barrier_semaphore()

    @pl.loop(1, devices)
    def _(j):
        other = (me + j) % devices
        pl.semaphore_signal(barrier, inc=1, device_id={"lon": other // lat_count, "lat": other % lat_count},
                            device_id_type=MESH_ID)

    def remote(src, dst, s, r, to_lat, to_lon):
        return pltpu.make_async_remote_copy(
            src, dst, s, r, device_id={"lon": to_lon, "lat": to_lat}, device_id_type=MESH_ID)

    middle = lon_count // 2 * lat_count

    def hand_over(k, n):
        shift = n + n // middle
        to_lon = lax.rem(lon + lon_count // 2 + shift // lat_count, lon_count)
        to_lat = lax.rem(lat + shift % lat_count, lat_count)
        other = to_lon * lat_count + to_lat
        return remote(SB.at[k, pl.ds(other * block, block)], GOT.at[k, pl.ds(me * block, block)],
                      obs_s.at[k, n], obs_r.at[k, n], to_lat, to_lon)

    def pk_lon():
        return (remote(PK.at[:, pl.ds(2, rows), tail], PK.at[:, pl.ds(2, rows), before], pk_s.at[0], pk_r.at[0], lat, east),
                remote(PK.at[:, pl.ds(2, rows), head], PK.at[:, pl.ds(2, rows), after], pk_s.at[1], pk_r.at[1], lat, west))

    def pk_piece(n, where):
        src, dst, to_lon = ((own, own, lon), (tail, before, east), (head, after, west))[n]
        srcs, dsts, to_lat, m = {
            "near": (PK.at[1, rows + 1, src], PK.at[1, 1, dst], down, 2),
            "far": (PK.at[1, rows, src], PK.at[1, 0, dst], down, 5),
            "side": (PK.at[0, rows + 1, src], PK.at[0, 1, dst], down, 8),
            "up": (PK.at[:, 2, src], PK.at[:, rows + 2, dst], up, 11)}[where]
        return remote(srcs, dsts, pk_s.at[m + n], pk_r.at[m + n], to_lat, to_lon)

    def lon_halo(X, n, m):
        return (remote(X.at[n, :, inner, tail], X.at[n, :, inner, before], lon_s.at[m, 0], lon_r.at[m, 0], lat, east),
                remote(X.at[n, :, inner, head], X.at[n, :, inner, after], lon_s.at[m, 1], lon_r.at[m, 1], lat, west))

    def diag_up(X, at, m, n):
        src, dst, to_lon = ((tail, before, east), (head, after, west))[n]
        return remote(X.at[at, :, pl.ds(top, 1 + ahead), src], X.at[at, :, pl.ds(below, 1 + ahead), dst],
                      diag_s.at[m, n], diag_r.at[m, n], up, to_lon)

    def diag_down(X, at, m, n):
        src, dst, to_lon = ((tail, before, east), (head, after, west))[n]
        return remote(X.at[at, :, pl.ds(bottom - ahead, 1 + ahead), src], X.at[at, :, pl.ds(above - ahead, 1 + ahead), dst],
                      diag_s.at[m, 2 + n], diag_r.at[m, 2 + n], down, to_lon)

    def row_up(X, at, m, g, d):
        return remote(X.at[at, g, top + d, own], X.at[at, g, below + d, own],
                      row_s.at[m, g, d, 0], row_r.at[m, g, d, 0], up, lon)

    def row_down(X, at, m, g, d):
        return remote(X.at[at, g, bottom - d, own], X.at[at, g, above - d, own],
                      row_s.at[m, g, d, 1], row_r.at[m, g, d, 1], down, lon)

    margin = total - 2 - ahead
    some = pl.ds(PAD - margin, width + 2 * margin)

    def lat_up(X, m, s, g):
        n = slot(s)
        return remote(X.at[n, g, top + ahead, some], X.at[n, g, below + ahead, some],
                      lat_s.at[m, s, g, 0], lat_r.at[m, s, g, 0], up, lon)

    def lat_down(X, m, s, g):
        n = slot(s)
        return remote(X.at[n, g, bottom - ahead, some], X.at[n, g, above - ahead, some],
                      lat_s.at[m, s, g, 1], lat_r.at[m, s, g, 1], down, lon)

    def start_up_down(upward, downward):
        @pl.when(has_up)
        def _():
            for copy in upward:
                copy().start()

        @pl.when(has_down)
        def _():
            for copy in downward:
                copy().start()

    def start_diagonals(X, at, m):
        start_up_down([partial(diag_up, X, at, m, n) for n in range(2)],
                      [partial(diag_down, X, at, m, n) for n in range(2)])

    def start_rows(X, at, m, d):
        @pl.loop(0, groups)
        def _(g):
            start_up_down([lambda: row_up(X, at, m, g, d)], [lambda: row_down(X, at, m, g, d)])

    def wait_rows(upward, downward):
        @pl.when(has_down)
        def _():
            upward().wait_recv()
            downward().wait_send()

        @pl.when(has_up)
        def _():
            downward().wait_recv()
            upward().wait_send()

    loads[0].wait()
    loads[1].wait()
    for i in range(2):
        for r in range(rows):
            w = winds[pl.ds(i * levels * rows + r, levels, stride=rows), :] * 0.5
            d = diff[pl.ds(r, 1), :]
            PK[i, r + 2, own, :] = jnp.concatenate([w + d, w - d], axis=0).T

    @pl.loop(0, groups)
    def _(g):
        state_load(g).wait()
        for r in range(rows):
            H[0, g, r + top, own, :] = state[pl.ds(g * LANES * rows + r, LANES, stride=rows), :].T

    edge = jnp.zeros((span, LANES), jnp.float32)

    @pl.when(jnp.logical_not(has_up))
    def _():
        PK[1, 1, wide, :] = edge

    def clear(first):
        @pl.loop(0, (RING + 1 if lead else min(total, RING)) * groups)
        def _(n):
            for X in (H, Y):
                for r in range(first, first + 1 + ahead):
                    X[n // groups, n % groups, r, wide, :] = edge

    @pl.when(jnp.logical_not(has_up))
    def _():
        clear(above - ahead)

    @pl.when(jnp.logical_not(has_down))
    def _():
        clear(below)

    pl.semaphore_wait(barrier, devices - 1)

    for copy in pk_lon():
        copy.start()
    start_up_down((), [partial(pk_piece, n, "near") for n in range(3)])
    for copy in lon_halo(H, 0, 0):
        copy.start()
    start_diagonals(H, 0, 0)
    start_rows(H, 0, 0, 0)
    if lead:
        start_up_down([partial(pk_piece, n, "up") for n in range(3)],
                      [partial(pk_piece, n, w) for w in ("side", "far") for n in range(3)])
        start_rows(H, 0, 0, 1)

    for load in loads[3:]:
        load.start()
    loads[2].wait()

    @pl.loop(0, slots)
    def _(k):
        for c in range(capacity):
            for h in range(chunks):
                SB[k, pl.ds(c * chunks + h, devices, stride=block), :] = obs[k, c, :, pl.ds(h * LANES, LANES)]
        for c in range(capacity * chunks, block):
            SB[k, pl.ds(c, devices, stride=block), :] = jnp.zeros((devices, LANES), jnp.float32)
        GOT[k, pl.ds(me * block, block), :] = SB[k, pl.ds(me * block, block), :]

    @pl.loop(0, slots * (devices - 1))
    def _(n):
        hand_over(n // (devices - 1), n % (devices - 1)).start()

    loads[3].wait()
    loads[4].wait()
    part = channels // 7

    @pl.loop(0, 14)
    def _(n):
        at = pl.ds(n % 7 * part, part)
        high, low = split2(tables[n // 7, at, :])
        TB[n // 7, at, pl.ds(0, prof)] = high
        TB[n // 7, at, pl.ds(prof, prof)] = low

    for copy in pk_lon():
        copy.wait_recv()

    @pl.when(has_up)
    def _():
        for n in range(3):
            pk_piece(n, "near").wait_recv()

    lower = lax.broadcasted_iota(jnp.int32, (span, LANES), 1) < levels

    def unpack(v):
        other = pltpu.roll(v, levels, 1)
        return jnp.where(lower, v, other), jnp.where(lower, other, v)

    def fill(C, q, signs, guard):
        a, b = unpack(PK[0, q + 1, wide, :])
        aw, bw = unpack(PK[0, q + 1, pl.ds(PAD - EXT - 1, span), :])
        al, bl = unpack(PK[1, q + 1, wide, :])
        au, bu = unpack(PK[1, q, wide, :])
        real = jnp.logical_and(jnp.logical_or(q > 0, has_up), jnp.logical_or(q <= rows, has_down))
        values = (-b, aw, -bl, au) if signs else (a, -bw, al, -bu)
        for n, v in enumerate((1.0 - a + bw - al + bu,) + values):
            C[n, q] = jnp.where(real, v, 0.0) if guard else v

    @pl.loop(1, rows + 1)
    def _(q):
        fill(F, q, True, False)

    first_count = steps_ref[0]
    second_count = steps_ref[1]
    kept = min(MAXSTEP, total - 1)

    def advance(X, C, src, dst, g, which, flag):
        for c in range(0, span, COLS):
            at = pl.ds(PAD - EXT + c, COLS)
            cat = pl.ds(c, COLS)
            row = {n: X[src, g, n, at, :] for n in sorted({r + d for r in which for d in (-1, 0, 1)})}
            for r in which:
                new = C[0, r - top + 1, cat, :] * row[r]
                new = new + C[3, r - top + 1, cat, :] * row[r + 1]
                new = new + C[4, r - top + 1, cat, :] * row[r - 1]
                new = new + C[1, r - top + 1, cat, :] * X[src, g, r, pl.ds(PAD - EXT + c + 1, COLS), :]
                new = new + C[2, r - top + 1, cat, :] * X[src, g, r, pl.ds(PAD - EXT + c - 1, COLS), :]
                if flag is not None:
                    new = new + jnp.where(flag, Y[RING, g, r, at, :], 0.0)
                X[dst, g, r, at, :] = new

    sent = tuple(sorted({top + ahead, bottom - ahead}))
    kept_rows = tuple(r for r in range(top, bottom + 1) if r not in sent)

    def turn(X, C, m, s, g, count=None):
        here, there = slot(s), slot(s + 1)
        flag = None if count is None else s + 1 == count

        @pl.when(s == 0)
        def _():
            wait_rows(lambda: row_up(X, 0, m, g, 0), lambda: row_down(X, 0, m, g, 0))

        @pl.when(s > ahead)
        def _():
            wait_rows(lambda: lat_up(X, m, s - ahead, g), lambda: lat_down(X, m, s - ahead, g))

        if lead:
            @pl.when(s == 1)
            def _():
                wait_rows(lambda: row_up(X, 0, m, g, 1), lambda: row_down(X, 0, m, g, 1))

            @pl.when(s > 0)
            def _():
                advance(X, C, slot(s + RING - 1), here, g, (above, below), None if count is None else s == count)

        advance(X, C, here, there, g, sent, flag)

        @pl.when(s < total - 1 - ahead)
        def _():
            start_up_down([lambda: lat_up(X, m, s + 1, g)], [lambda: lat_down(X, m, s + 1, g)])

        advance(X, C, here, there, g, kept_rows, flag)

        if count is None:
            @pl.when(s < kept)
            def _():
                for r in range(top, bottom + 1):
                    H[RING, g, r, own, :] = jnp.where(s < first_count, H[there, g, r, own, :], H[RING, g, r, own, :])

    def wait_edges(X, at, m):
        for copy in lon_halo(X, at, m):
            copy.wait()
        if m == 2 and not lead:
            return

        @pl.when(has_down)
        def _():
            for n in range(2):
                diag_up(X, at, m, n).wait_recv()
                diag_down(X, at, m, n).wait_send()

        @pl.when(has_up)
        def _():
            for n in range(2):
                diag_down(X, at, m, n).wait_recv()
                diag_up(X, at, m, n).wait_send()

    def select(n):
        b = n % chunks
        column = jnp.broadcast_to(chan_ref[pl.ds(b, 1), :].astype(jnp.float32), (LANES, LANES)).T
        column = jnp.concatenate([column] * -(-channels // LANES), axis=1)[:, :channels]
        picker = (column == lax.broadcasted_iota(jnp.int32, (LANES, channels), 1).astype(jnp.float32)).astype(
            jnp.float32).astype(jnp.bfloat16)
        AE[pl.ds(n * LANES, LANES), :] = dot(picker, TB[n // chunks]).astype(jnp.bfloat16)

        @pl.when(n < chunks)
        def _():
            weights = jnp.concatenate(
                [jnp.broadcast_to(v, (8, channels)) for v in split3(weight_ref[...].reshape(1, channels))], axis=0)
            w = dot(weights, picker, LAST)
            WS[pl.ds(b, 1), :] = w[0:1] + w[8:9] + w[16:17]

    earlier = lax.broadcasted_iota(jnp.int32, (soundings, soundings), 0) < lax.broadcasted_iota(
        jnp.int32, (soundings, soundings), 1)

    def collect(k):
        @pl.loop(0, devices - 1)
        def _(n):
            hand_over(k, n).wait_recv()

        owner = owner_ref[k]
        spread = jnp.broadcast_to(owner.astype(jnp.float32), (soundings, soundings))
        same = jnp.logical_and(spread.T == spread, earlier)
        rank = jnp.sum(same.astype(jnp.float32), axis=0, keepdims=True).astype(jnp.int32)
        places = block // chunks
        source = one_hot(owner * places + rank, devices * places)
        for h in range(chunks):
            got = dot(source, jnp.concatenate(split2(GOT[k, pl.ds(h, devices * places, stride=chunks), :]), axis=1), FIRST)
            WN[k, :, pl.ds(h * LANES, LANES)] = got[:, :LANES] + got[:, LANES:]

    def observe(k):
        placed = one_hot(cell_ref[pl.ds(k, 1), :], cells)
        weight = jnp.concatenate([WS[b:b + 1, :] for b in range(chunks)], axis=1)
        high, low = [], []
        for g in range(groups):
            field = H[jnp.where(k == 0, RING, total % RING), g, inner, own, :].reshape(cells, LANES)
            taken = dot(placed, jnp.concatenate(split2(field), axis=1), FIRST).astype(jnp.bfloat16)
            high.append(taken[:, :LANES])
            low.append(taken[:, LANES:])
        high = jnp.concatenate(high, axis=1)
        low = jnp.concatenate(low, axis=1)
        table, rest = AE[:, pl.ds(0, prof)], AE[:, pl.ds(prof, prof)]
        both = dot(jnp.concatenate([high, low], axis=0), table, LAST)
        both = both[:soundings] + both[soundings:] + dot(high, rest, LAST)
        optical, bright = both[:, :used], both[:, used:]
        small = jnp.exp(-jnp.abs(optical))
        inv = 1.0 / (1.0 + small)
        passed = jnp.where(optical > 0, small, 1.0) * inv
        slope = jnp.where(optical > 0, 1.0, small) * inv
        y = passed * bright
        departure = weight * (y - WN[k])
        high, low = split2(jnp.concatenate([-(departure * y) * slope, departure * passed], axis=1))
        both = dot(jnp.concatenate([high, low], axis=0), table)
        back = both[:soundings] + both[soundings:] + dot(high, rest)
        back = jnp.concatenate(split2(back), axis=0)
        placed = jnp.concatenate([placed, placed], axis=1)
        target = jnp.where(k == 0, RING, 0)
        for g in range(groups):
            Y[target, g, inner, own, :] = dot(placed, back[:, g * LANES:(g + 1) * LANES]).reshape(rows, width, LANES)

        for copy in lon_halo(Y, target, 2 - k):
            copy.start()

        if lead:
            start_diagonals(Y, target, 2 - k)
            start_rows(Y, target, 2 - k, 0)

        @pl.when(k > 0)
        def _():
            if lead:
                start_rows(Y, 0, 1, 1)
            else:
                start_diagonals(Y, 0, 1)
                start_rows(Y, 0, 1, 0)

    wait_edges(H, 0, 0)
    turns = total * groups
    early = (total - 1 - ahead) * groups - 1
    ready = turns if total < 4 else turns - 2

    @pl.loop(0, turns + 1)
    def _(it):
        if lead:
            @pl.when(it == groups)
            def _():
                @pl.when(has_down)
                def _():
                    for n in range(3):
                        pk_piece(n, "up").wait_recv()
                        for w in ("near", "side", "far"):
                            pk_piece(n, w).wait_send()

                @pl.when(has_up)
                def _():
                    for n in range(3):
                        pk_piece(n, "up").wait_send()
                        for w in ("side", "far"):
                            pk_piece(n, w).wait_recv()

                fill(F, 0, True, True)
                fill(F, rows + 1, True, True)

        @pl.when(it < turns)
        def _():
            turn(H, F, 0, lax.div(it, groups), lax.rem(it, groups))

        began = groups * ahead

        @pl.when(jnp.logical_and(it > began, it <= began + rows + 2 * ahead))
        def _():
            fill(B, it - began - ahead, False, lead)

        for n in range(-(-2 * chunks // (kept * groups))):
            at = it + n * kept * groups

            @pl.when(jnp.logical_and(it < kept * groups, at < 2 * chunks))
            def _():
                select(at)

        @pl.when(jnp.logical_or(it == early, it == ready))
        def _():
            collect((it == ready).astype(jnp.int32))

        @pl.when(jnp.logical_or(it == early, it == turns))
        def _():
            observe((it == turns).astype(jnp.int32))

    @pl.loop(0, slots * (devices - 1))
    def _(n):
        hand_over(n // (devices - 1), n % (devices - 1)).wait_send()

    for copy in pk_lon():
        copy.wait_send()

    wait_edges(Y, 0, 1)
    wait_edges(Y, RING, 2)
    if lead:
        @pl.loop(0, groups)
        def _(g):
            wait_rows(lambda: row_up(Y, RING, 2, g, 0), lambda: row_down(Y, RING, 2, g, 0))
    else:
        @pl.when(has_down)
        def _():
            for n in range(3):
                pk_piece(n, "near").wait_send()

    @pl.loop(0, turns)
    def _(it):
        s = lax.div(it, groups)
        g = lax.rem(it, groups)
        turn(Y, B, 1, s, g, second_count)

        @pl.when(s == total - 1)
        def _():
            for r in range(rows):
                out_ref[pl.ds(g * LANES * rows + r, LANES, stride=rows), :] = Y[total % RING, g, r + top, own, :].T


def whole_call(lat_count, lon_count, total, step_counts, state, winds, diffusivity, by_rank, absorb, emit,
               cells, owners, channel_list, weight):
    rows, width = diffusivity.shape
    groups = state.shape[0] // (rows * LANES)
    slots, capacity, devices, used = by_rank.shape
    channels, prof = absorb.shape
    block = -(-capacity * (used // LANES) // 8) * 8
    wide = width + 2 * PAD
    span = width + 2 * EXT
    lead = int(total - 2 >= MAXSTEP)
    held = rows + 2 + 2 * lead
    vmem = pl.BlockSpec(memory_space=pltpu.VMEM)
    hbm = pl.BlockSpec(memory_space=pl.ANY)
    f32, bf16 = jnp.float32, jnp.bfloat16
    dma = pltpu.SemaphoreType.DMA
    scratch = [
        pltpu.VMEM(state.shape, f32), pltpu.VMEM(winds.shape, f32), pltpu.VMEM(diffusivity.shape, f32),
        pltpu.VMEM(by_rank.shape, f32), pltpu.VMEM((2, channels, prof), f32),
        pltpu.VMEM((2, channels, 2 * prof), bf16), pltpu.VMEM((2 * used, 2 * prof), bf16),
        pltpu.VMEM((used // LANES, LANES), f32),
        pltpu.VMEM((RING + 1, groups, held, wide, LANES), f32),
        pltpu.VMEM((RING + 1, groups, held, wide, LANES), f32),
        pltpu.VMEM((5, rows + 2, span, LANES), f32), pltpu.VMEM((5, rows + 2, span, LANES), f32),
        pltpu.VMEM((2, rows + 4, wide, LANES), f32),
        pltpu.VMEM((slots, devices * block, LANES), f32), pltpu.VMEM((slots, devices * block, LANES), f32),
        pltpu.VMEM((slots, cells.shape[1], used), f32),
        dma((5,)), dma((groups,)), *[dma((14 if lead else 5,))] * 2, *[dma((2 + lead, groups, 1 + lead, 2))] * 2,
        *[dma((3, 2))] * 2, *[dma((2 + lead, 4))] * 2, *[dma((2, total, groups, 2))] * 2,
        dma((slots, devices)), dma((slots, devices)),
    ]
    return pl.pallas_call(
        partial(whole_kernel, total, lat_count, lon_count),
        out_shape=jax.ShapeDtypeStruct(state.shape, f32),
        in_specs=[pl.BlockSpec(memory_space=pltpu.SMEM)] + [hbm] * 6 + [vmem] * 4,
        out_specs=vmem,
        scratch_shapes=scratch,
        compiler_params=pltpu.CompilerParams(
            collective_id=total, has_side_effects=True, vmem_limit_bytes=60 << 20),
        name="whole",
    )(step_counts, state, winds, diffusivity, by_rank, absorb, emit, cells, owners, channel_list, weight)


def form_kernel(slots, steps_ref, out_ref):
    out_ref[0] = steps_ref[0] + steps_ref[1] - slots


def form_of(step_counts, slots):
    smem = pl.BlockSpec(memory_space=pltpu.SMEM)
    return pl.pallas_call(partial(form_kernel, slots), out_shape=jax.ShapeDtypeStruct((1,), jnp.int32),
                          in_specs=[smem], out_specs=smem, name="form")(step_counts)


def per_device(lat_count, lon_count, state, winds, diffusivity, sounding_cell, sounding_owner,
               step_counts, channel_list, absorb_table, emit_table, obs_weight, observed):
    width = state.shape[-1]
    operands = (
        step_counts, state.reshape(-1, width), winds.reshape(-1, width), diffusivity,
        jnp.transpose(observed[:, 0], (0, 2, 1, 3)), absorb_table.T, emit_table.T,
        sounding_cell, jnp.transpose(sounding_owner, (0, 2, 1)), channel_list.reshape(-1, LANES),
        obs_weight)
    slots = step_counts.shape[0]
    branches = [partial(whole_call, lat_count, lon_count, n) for n in range(slots, slots * MAXSTEP + 1)]
    return lax.switch(form_of(step_counts, slots)[0], branches, *operands).reshape(state.shape)


def solution(mesh):
    return jax.shard_map(
        partial(per_device, mesh.shape["lat"], mesh.shape["lon"]),
        mesh=mesh,
        in_specs=(
            P(None, None, "lat", "lon"),
            P(None, None, "lat", "lon"),
            P("lat", "lon"),
            P(None, ("lon", "lat")),
            P(None, ("lon", "lat"), None),
            P(),
            P(),
            P(),
            P(),
            P(),
            P(None, ("lon", "lat"), None, None, None),
        ),
        out_specs=P(None, None, "lat", "lon"),
        check_vma=False,
    )
```

```python
from functools import partial

import jax
import jax.numpy as jnp
from jax import lax
from jax.experimental import pallas as pl
from jax.experimental.pallas import tpu as pltpu
from jax.sharding import PartitionSpec as P

MAXSTEP = 4
LANES = 128
EXT = 8
PAD = 16
COLS = 24
RING = 4
MESH_ID = pl.DeviceIdType.MESH
FIRST = ((0,), (0,))
LAST = ((1,), (1,))


def split2(v):
    high = v.astype(jnp.bfloat16)
    return high, (v - high.astype(jnp.float32)).astype(jnp.bfloat16)


def split3(v):
    high = v.astype(jnp.bfloat16)
    rest = v - high.astype(jnp.float32)
    mid = rest.astype(jnp.bfloat16)
    return high, mid, (rest - mid.astype(jnp.float32)).astype(jnp.bfloat16)


def dot(a, b, dims=((1,), (0,))):
    return lax.dot_general(a, b, (dims, ((), ())), preferred_element_type=jnp.float32)


def one_hot(row, size):
    return (row == lax.broadcasted_iota(jnp.int32, (size, row.shape[1]), 0)).astype(
        jnp.float32).astype(jnp.bfloat16)


def whole_kernel(total, lat_count, lon_count, *refs):
    (steps_ref, state_hbm, winds_hbm, diff_hbm, obs_hbm, absorb_hbm, emit_hbm, cell_ref, owner_ref, chan_ref,
     weight_ref, out_ref,
     state, winds, diff, obs, tables, TB, AE, WS, H, Y, F, B, PK, SB, GOT, WN,
     local_sem, state_sem, pk_s, pk_r, row_s, row_r, lon_s, lon_r, diag_s, diag_r, lat_s, lat_r, obs_s, obs_r) = refs
    groups, rows = H.shape[1], diff.shape[0]
    width = state.shape[1]
    span = width + 2 * EXT
    levels = winds.shape[0] // (2 * rows)
    devices = lat_count * lon_count
    slots, capacity, _, used = obs.shape
    chunks = used // LANES
    block = SB.shape[1] // devices
    channels, prof = tables.shape[1:]
    cells = rows * width
    soundings = cell_ref.shape[1]
    lat = lax.axis_index("lat")
    lon = lax.axis_index("lon")
    me = lon * lat_count + lat
    east = lax.rem(lon + 1, lon_count)
    west = lax.rem(lon + lon_count - 1, lon_count)
    has_up = lat > 0
    has_down = lat < lat_count - 1
    up, down = lat - 1, lat + 1
    own = pl.ds(PAD, width)
    wide = pl.ds(PAD - EXT, span)
    head, tail = pl.ds(PAD, EXT), pl.ds(PAD + width - EXT, EXT)
    before, after = pl.ds(PAD - EXT, EXT), pl.ds(PAD + width, EXT)
    lead = total - 2 >= MAXSTEP
    ahead = 1 if lead else 0

    top, bottom, above, below = 1 + ahead, rows + ahead, ahead, rows + 1 + ahead
    inner = pl.ds(top, rows)

    def slot(n):
        return n if total < RING else lax.rem(n, RING)

    loads = [pltpu.make_async_copy(src, dst, local_sem.at[n]) for n, (src, dst) in enumerate((
        (winds_hbm, winds), (diff_hbm, diff), (obs_hbm, obs),
        (absorb_hbm, tables.at[0]), (emit_hbm, tables.at[1])))]
    for load in loads[:2]:
        load.start()

    def state_load(g):
        at = pl.ds(g * LANES * rows, LANES * rows)
        return pltpu.make_async_copy(state_hbm.at[at], state.at[at], state_sem.at[g])

    @pl.loop(0, groups)
    def _(g):
        state_load(g).start()

    loads[2].start()
    barrier = pltpu.get_barrier_semaphore()

    @pl.loop(1, devices)
    def _(j):
        other = (me + j) % devices
        pl.semaphore_signal(barrier, inc=1, device_id={"lon": other // lat_count, "lat": other % lat_count},
                            device_id_type=MESH_ID)

    def remote(src, dst, s, r, to_lat, to_lon):
        return pltpu.make_async_remote_copy(
            src, dst, s, r, device_id={"lon": to_lon, "lat": to_lat}, device_id_type=MESH_ID)

    middle = lon_count // 2 * lat_count

    def hand_over(k, n):
        shift = n + n // middle
        to_lon = lax.rem(lon + lon_count // 2 + shift // lat_count, lon_count)
        to_lat = lax.rem(lat + shift % lat_count, lat_count)
        other = to_lon * lat_count + to_lat
        return remote(SB.at[k, pl.ds(other * block, block)], GOT.at[k, pl.ds(me * block, block)],
                      obs_s.at[k], obs_r.at[k], to_lat, to_lon)

    def handed(k):
        most = pl.ds(0, (devices - 1) * block)
        return remote(SB.at[k, most], GOT.at[k, most], obs_s.at[k], obs_r.at[k], lat, east)

    def pk_lon():
        return (remote(PK.at[:, pl.ds(2, rows), tail], PK.at[:, pl.ds(2, rows), before], pk_s.at[0], pk_r.at[0], lat, east),
                remote(PK.at[:, pl.ds(2, rows), head], PK.at[:, pl.ds(2, rows), after], pk_s.at[1], pk_r.at[1], lat, west))

    def pk_piece(n, where):
        src, dst, to_lon = ((own, own, lon), (tail, before, east), (head, after, west))[n]
        srcs, dsts, to_lat, m = {
            "near": (PK.at[1, rows + 1, src], PK.at[1, 1, dst], down, 2),
            "far": (PK.at[1, rows, src], PK.at[1, 0, dst], down, 5),
            "side": (PK.at[0, rows + 1, src], PK.at[0, 1, dst], down, 8),
            "up": (PK.at[:, 2, src], PK.at[:, rows + 2, dst], up, 11)}[where]
        return remote(srcs, dsts, pk_s.at[m + n], pk_r.at[m + n], to_lat, to_lon)

    def lon_halo(X, n, m):
        return (remote(X.at[n, :, inner, tail], X.at[n, :, inner, before], lon_s.at[m, 0], lon_r.at[m, 0], lat, east),
                remote(X.at[n, :, inner, head], X.at[n, :, inner, after], lon_s.at[m, 1], lon_r.at[m, 1], lat, west))

    def diag_up(X, at, m, n):
        src, dst, to_lon = ((tail, before, east), (head, after, west))[n]
        return remote(X.at[at, :, pl.ds(top, 1 + ahead), src], X.at[at, :, pl.ds(below, 1 + ahead), dst],
                      diag_s.at[m, n], diag_r.at[m, n], up, to_lon)

    def diag_down(X, at, m, n):
        src, dst, to_lon = ((tail, before, east), (head, after, west))[n]
        return remote(X.at[at, :, pl.ds(bottom - ahead, 1 + ahead), src], X.at[at, :, pl.ds(above - ahead, 1 + ahead), dst],
                      diag_s.at[m, 2 + n], diag_r.at[m, 2 + n], down, to_lon)

    def row_up(X, at, m, g, d):
        return remote(X.at[at, g, top + d, own], X.at[at, g, below + d, own],
                      row_s.at[m, g, d, 0], row_r.at[m, g, d, 0], up, lon)

    def row_down(X, at, m, g, d):
        return remote(X.at[at, g, bottom - d, own], X.at[at, g, above - d, own],
                      row_s.at[m, g, d, 1], row_r.at[m, g, d, 1], down, lon)

    margin = total - 2 - ahead
    some = pl.ds(PAD - margin, width + 2 * margin)

    def lat_up(X, m, s, g):
        n = slot(s)
        return remote(X.at[n, g, top + ahead, some], X.at[n, g, below + ahead, some],
                      lat_s.at[m, s, g, 0], lat_r.at[m, s, g, 0], up, lon)

    def lat_down(X, m, s, g):
        n = slot(s)
        return remote(X.at[n, g, bottom - ahead, some], X.at[n, g, above - ahead, some],
                      lat_s.at[m, s, g, 1], lat_r.at[m, s, g, 1], down, lon)

    def start_up_down(upward, downward):
        @pl.when(has_up)
        def _():
            for copy in upward:
                copy().start()

        @pl.when(has_down)
        def _():
            for copy in downward:
                copy().start()

    def start_diagonals(X, at, m):
        start_up_down([partial(diag_up, X, at, m, n) for n in range(2)],
                      [partial(diag_down, X, at, m, n) for n in range(2)])

    def start_rows(X, at, m, d):
        @pl.loop(0, groups)
        def _(g):
            start_up_down([lambda: row_up(X, at, m, g, d)], [lambda: row_down(X, at, m, g, d)])

    def wait_rows(upward, downward):
        @pl.when(has_down)
        def _():
            upward().wait_recv()
            downward().wait_send()

        @pl.when(has_up)
        def _():
            downward().wait_recv()
            upward().wait_send()

    loads[0].wait()
    loads[1].wait()
    for i in range(2):
        for r in range(rows):
            w = winds[pl.ds(i * levels * rows + r, levels, stride=rows), :] * 0.5
            d = diff[pl.ds(r, 1), :]
            PK[i, r + 2, own, :] = jnp.concatenate([w + d, w - d], axis=0).T

    @pl.loop(0, groups)
    def _(g):
        state_load(g).wait()
        for r in range(rows):
            H[0, g, r + top, own, :] = state[pl.ds(g * LANES * rows + r, LANES, stride=rows), :].T

    edge = jnp.zeros((span, LANES), jnp.float32)

    @pl.when(jnp.logical_not(has_up))
    def _():
        PK[1, 1, wide, :] = edge

    def clear(first):
        @pl.loop(0, (RING + 1 if lead else min(total, RING)) * groups)
        def _(n):
            for X in (H, Y):
                for r in range(first, first + 1 + ahead):
                    X[n // groups, n % groups, r, wide, :] = edge

    @pl.when(jnp.logical_not(has_up))
    def _():
        clear(above - ahead)

    @pl.when(jnp.logical_not(has_down))
    def _():
        clear(below)

    pl.semaphore_wait(barrier, devices - 1)

    for copy in pk_lon():
        copy.start()
    start_up_down((), [partial(pk_piece, n, "near") for n in range(3)])
    for copy in lon_halo(H, 0, 0):
        copy.start()
    start_diagonals(H, 0, 0)
    start_rows(H, 0, 0, 0)
    if lead:
        start_up_down([partial(pk_piece, n, "up") for n in range(3)],
                      [partial(pk_piece, n, w) for w in ("side", "far") for n in range(3)])
        start_rows(H, 0, 0, 1)

    for load in loads[3:]:
        load.start()
    loads[2].wait()

    @pl.loop(0, slots)
    def _(k):
        for c in range(capacity):
            for h in range(chunks):
                SB[k, pl.ds(c * chunks + h, devices, stride=block), :] = obs[k, c, :, pl.ds(h * LANES, LANES)]
        for c in range(capacity * chunks, block):
            SB[k, pl.ds(c, devices, stride=block), :] = jnp.zeros((devices, LANES), jnp.float32)
        GOT[k, pl.ds(me * block, block), :] = SB[k, pl.ds(me * block, block), :]

    @pl.loop(0, slots * (devices - 1))
    def _(n):
        hand_over(n // (devices - 1), n % (devices - 1)).start()

    loads[3].wait()
    loads[4].wait()
    part = channels // 7

    @pl.loop(0, 14)
    def _(n):
        at = pl.ds(n % 7 * part, part)
        high, low = split2(tables[n // 7, at, :])
        TB[n // 7, at, pl.ds(0, prof)] = high
        TB[n // 7, at, pl.ds(prof, prof)] = low

    for copy in pk_lon():
        copy.wait_recv()

    @pl.when(has_up)
    def _():
        for n in range(3):
            pk_piece(n, "near").wait_recv()

    lower = lax.broadcasted_iota(jnp.int32, (span, LANES), 1) < levels

    def unpack(v):
        other = pltpu.roll(v, levels, 1)
        return jnp.where(lower, v, other), jnp.where(lower, other, v)

    def fill(C, q, signs, guard):
        a, b = unpack(PK[0, q + 1, wide, :])
        aw, bw = unpack(PK[0, q + 1, pl.ds(PAD - EXT - 1, span), :])
        al, bl = unpack(PK[1, q + 1, wide, :])
        au, bu = unpack(PK[1, q, wide, :])
        real = jnp.logical_and(jnp.logical_or(q > 0, has_up), jnp.logical_or(q <= rows, has_down))
        values = (-b, aw, -bl, au) if signs else (a, -bw, al, -bu)
        for n, v in enumerate((1.0 - a + bw - al + bu,) + values):
            C[n, q] = jnp.where(real, v, 0.0) if guard else v

    @pl.loop(1, rows + 1)
    def _(q):
        fill(F, q, True, False)

    first_count = steps_ref[0]
    second_count = steps_ref[1]
    kept = min(MAXSTEP, total - 1)

    def advance(X, C, src, dst, g, which, flag):
        for c in range(0, span, COLS):
            at = pl.ds(PAD - EXT + c, COLS)
            cat = pl.ds(c, COLS)
            row = {n: X[src, g, n, at, :] for n in sorted({r + d for r in which for d in (-1, 0, 1)})}
            for r in which:
                new = C[0, r - top + 1, cat, :] * row[r]
                new = new + C[3, r - top + 1, cat, :] * row[r + 1]
                new = new + C[4, r - top + 1, cat, :] * row[r - 1]
                new = new + C[1, r - top + 1, cat, :] * X[src, g, r, pl.ds(PAD - EXT + c + 1, COLS), :]
                new = new + C[2, r - top + 1, cat, :] * X[src, g, r, pl.ds(PAD - EXT + c - 1, COLS), :]
                if flag is not None:
                    new = new + jnp.where(flag, Y[RING, g, r, at, :], 0.0)
                X[dst, g, r, at, :] = new

    sent = tuple(sorted({top + ahead, bottom - ahead}))
    kept_rows = tuple(r for r in range(top, bottom + 1) if r not in sent)

    def turn(X, C, m, s, g, count=None):
        here, there = slot(s), slot(s + 1)
        flag = None if count is None else s + 1 == count

        @pl.when(s == 0)
        def _():
            wait_rows(lambda: row_up(X, 0, m, g, 0), lambda: row_down(X, 0, m, g, 0))

        @pl.when(s > ahead)
        def _():
            wait_rows(lambda: lat_up(X, m, s - ahead, g), lambda: lat_down(X, m, s - ahead, g))

        if lead:
            @pl.when(s == 1)
            def _():
                wait_rows(lambda: row_up(X, 0, m, g, 1), lambda: row_down(X, 0, m, g, 1))

            @pl.when(s > 0)
            def _():
                advance(X, C, slot(s + RING - 1), here, g, (above, below), None if count is None else s == count)

        advance(X, C, here, there, g, sent, flag)

        @pl.when(s < total - 1 - ahead)
        def _():
            start_up_down([lambda: lat_up(X, m, s + 1, g)], [lambda: lat_down(X, m, s + 1, g)])

        advance(X, C, here, there, g, kept_rows, flag)

        if count is None:
            @pl.when(s < kept)
            def _():
                for r in range(top, bottom + 1):
                    H[RING, g, r, own, :] = jnp.where(s < first_count, H[there, g, r, own, :], H[RING, g, r, own, :])

    def wait_edges(X, at, m):
        for copy in lon_halo(X, at, m):
            copy.wait()
        if m == 2 and not lead:
            return

        @pl.when(has_down)
        def _():
            for n in range(2):
                diag_up(X, at, m, n).wait_recv()
                diag_down(X, at, m, n).wait_send()

        @pl.when(has_up)
        def _():
            for n in range(2):
                diag_down(X, at, m, n).wait_recv()
                diag_up(X, at, m, n).wait_send()

    def select(n):
        b = n % chunks
        column = jnp.broadcast_to(chan_ref[pl.ds(b, 1), :].astype(jnp.float32), (LANES, LANES)).T
        column = jnp.concatenate([column] * -(-channels // LANES), axis=1)[:, :channels]
        picker = (column == lax.broadcasted_iota(jnp.int32, (LANES, channels), 1).astype(jnp.float32)).astype(
            jnp.float32).astype(jnp.bfloat16)
        AE[pl.ds(n * LANES, LANES), :] = dot(picker, TB[n // chunks]).astype(jnp.bfloat16)

        @pl.when(n < chunks)
        def _():
            weights = jnp.concatenate(
                [jnp.broadcast_to(v, (8, channels)) for v in split3(weight_ref[...].reshape(1, channels))], axis=0)
            w = dot(weights, picker, LAST)
            WS[pl.ds(b, 1), :] = w[0:1] + w[8:9] + w[16:17]

    earlier = lax.broadcasted_iota(jnp.int32, (soundings, soundings), 0) < lax.broadcasted_iota(
        jnp.int32, (soundings, soundings), 1)

    def collect(k):
        handed(k).wait_recv()
        owner = owner_ref[k]
        spread = jnp.broadcast_to(owner.astype(jnp.float32), (soundings, soundings))
        same = jnp.logical_and(spread.T == spread, earlier)
        rank = jnp.sum(same.astype(jnp.float32), axis=0, keepdims=True).astype(jnp.int32)
        places = block // chunks
        source = one_hot(owner * places + rank, devices * places)
        for h in range(chunks):
            got = dot(source, jnp.concatenate(split2(GOT[k, pl.ds(h, devices * places, stride=chunks), :]), axis=1), FIRST)
            WN[k, :, pl.ds(h * LANES, LANES)] = got[:, :LANES] + got[:, LANES:]

    def observe(k):
        placed = one_hot(cell_ref[pl.ds(k, 1), :], cells)
        weight = jnp.concatenate([WS[b:b + 1, :] for b in range(chunks)], axis=1)
        high, low = [], []
        for g in range(groups):
            field = H[jnp.where(k == 0, RING, total % RING), g, inner, own, :].reshape(cells, LANES)
            taken = dot(placed, jnp.concatenate(split2(field), axis=1), FIRST).astype(jnp.bfloat16)
            high.append(taken[:, :LANES])
            low.append(taken[:, LANES:])
        high = jnp.concatenate(high, axis=1)
        low = jnp.concatenate(low, axis=1)
        table, rest = AE[:, pl.ds(0, prof)], AE[:, pl.ds(prof, prof)]
        both = dot(jnp.concatenate([high, low], axis=0), table, LAST)
        both = both[:soundings] + both[soundings:] + dot(high, rest, LAST)
        optical, bright = both[:, :used], both[:, used:]
        small = jnp.exp(-jnp.abs(optical))
        inv = 1.0 / (1.0 + small)
        passed = jnp.where(optical > 0, small, 1.0) * inv
        slope = jnp.where(optical > 0, 1.0, small) * inv
        y = passed * bright
        departure = weight * (y - WN[k])
        high, low = split2(jnp.concatenate([-(departure * y) * slope, departure * passed], axis=1))
        both = dot(jnp.concatenate([high, low], axis=0), table)
        back = both[:soundings] + both[soundings:] + dot(high, rest)
        back = jnp.concatenate(split2(back), axis=0)
        placed = jnp.concatenate([placed, placed], axis=1)
        target = jnp.where(k == 0, RING, 0)
        for g in range(groups):
            Y[target, g, inner, own, :] = dot(placed, back[:, g * LANES:(g + 1) * LANES]).reshape(rows, width, LANES)

        for copy in lon_halo(Y, target, 2 - k):
            copy.start()

        if lead:
            start_diagonals(Y, target, 2 - k)
            start_rows(Y, target, 2 - k, 0)

        @pl.when(k > 0)
        def _():
            if lead:
                start_rows(Y, 0, 1, 1)
            else:
                start_diagonals(Y, 0, 1)
                start_rows(Y, 0, 1, 0)

    wait_edges(H, 0, 0)
    turns = total * groups
    early = (total - 1 - ahead) * groups - 1
    ready = turns if total < 4 else turns - 2

    @pl.loop(0, turns + 1)
    def _(it):
        if lead:
            @pl.when(it == groups)
            def _():
                @pl.when(has_down)
                def _():
                    for n in range(3):
                        pk_piece(n, "up").wait_recv()
                        for w in ("near", "side", "far"):
                            pk_piece(n, w).wait_send()

                @pl.when(has_up)
                def _():
                    for n in range(3):
                        pk_piece(n, "up").wait_send()
                        for w in ("side", "far"):
                            pk_piece(n, w).wait_recv()

                fill(F, 0, True, True)
                fill(F, rows + 1, True, True)

        @pl.when(it < turns)
        def _():
            turn(H, F, 0, lax.div(it, groups), lax.rem(it, groups))

        began = groups * ahead

        @pl.when(jnp.logical_and(it > began, it <= began + rows + 2 * ahead))
        def _():
            fill(B, it - began - ahead, False, lead)

        for n in range(-(-2 * chunks // (kept * groups))):
            at = it + n * kept * groups

            @pl.when(jnp.logical_and(it < kept * groups, at < 2 * chunks))
            def _():
                select(at)

        @pl.when(jnp.logical_or(it == early, it == ready))
        def _():
            collect((it == ready).astype(jnp.int32))

        @pl.when(jnp.logical_or(it == early, it == turns))
        def _():
            observe((it == turns).astype(jnp.int32))

    for k in range(slots):
        handed(k).wait_send()

    for copy in pk_lon():
        copy.wait_send()

    wait_edges(Y, 0, 1)
    wait_edges(Y, RING, 2)
    if lead:
        @pl.loop(0, groups)
        def _(g):
            wait_rows(lambda: row_up(Y, RING, 2, g, 0), lambda: row_down(Y, RING, 2, g, 0))
    else:
        @pl.when(has_down)
        def _():
            for n in range(3):
                pk_piece(n, "near").wait_send()

    @pl.loop(0, turns)
    def _(it):
        s = lax.div(it, groups)
        g = lax.rem(it, groups)
        turn(Y, B, 1, s, g, second_count)

        @pl.when(s == total - 1)
        def _():
            for r in range(rows):
                out_ref[pl.ds(g * LANES * rows + r, LANES, stride=rows), :] = Y[total % RING, g, r + top, own, :].T


def whole_call(lat_count, lon_count, total, step_counts, state, winds, diffusivity, by_rank, absorb, emit,
               cells, owners, channel_list, weight):
    rows, width = diffusivity.shape
    groups = state.shape[0] // (rows * LANES)
    slots, capacity, devices, used = by_rank.shape
    channels, prof = absorb.shape
    block = -(-capacity * (used // LANES) // 8) * 8
    wide = width + 2 * PAD
    span = width + 2 * EXT
    lead = int(total - 2 >= MAXSTEP)
    held = rows + 2 + 2 * lead
    vmem = pl.BlockSpec(memory_space=pltpu.VMEM)
    hbm = pl.BlockSpec(memory_space=pl.ANY)
    f32, bf16 = jnp.float32, jnp.bfloat16
    dma = pltpu.SemaphoreType.DMA
    scratch = [
        pltpu.VMEM(state.shape, f32), pltpu.VMEM(winds.shape, f32), pltpu.VMEM(diffusivity.shape, f32),
        pltpu.VMEM(by_rank.shape, f32), pltpu.VMEM((2, channels, prof), f32),
        pltpu.VMEM((2, channels, 2 * prof), bf16), pltpu.VMEM((2 * used, 2 * prof), bf16),
        pltpu.VMEM((used // LANES, LANES), f32),
        pltpu.VMEM((RING + 1, groups, held, wide, LANES), f32),
        pltpu.VMEM((RING + 1, groups, held, wide, LANES), f32),
        pltpu.VMEM((5, rows + 2, span, LANES), f32), pltpu.VMEM((5, rows + 2, span, LANES), f32),
        pltpu.VMEM((2, rows + 4, wide, LANES), f32),
        pltpu.VMEM((slots, devices * block, LANES), f32), pltpu.VMEM((slots, devices * block, LANES), f32),
        pltpu.VMEM((slots, cells.shape[1], used), f32),
        dma((5,)), dma((groups,)), *[dma((14 if lead else 5,))] * 2, *[dma((2 + lead, groups, 1 + lead, 2))] * 2,
        *[dma((3, 2))] * 2, *[dma((2 + lead, 4))] * 2, *[dma((2, total, groups, 2))] * 2,
        dma((slots,)), dma((slots,)),
    ]
    return pl.pallas_call(
        partial(whole_kernel, total, lat_count, lon_count),
        out_shape=jax.ShapeDtypeStruct(state.shape, f32),
        in_specs=[pl.BlockSpec(memory_space=pltpu.SMEM)] + [hbm] * 6 + [vmem] * 4,
        out_specs=vmem,
        scratch_shapes=scratch,
        compiler_params=pltpu.CompilerParams(
            collective_id=total, has_side_effects=True, vmem_limit_bytes=60 << 20),
        name="whole",
    )(step_counts, state, winds, diffusivity, by_rank, absorb, emit, cells, owners, channel_list, weight)


def form_kernel(slots, steps_ref, out_ref):
    out_ref[0] = steps_ref[0] + steps_ref[1] - slots


def form_of(step_counts, slots):
    smem = pl.BlockSpec(memory_space=pltpu.SMEM)
    return pl.pallas_call(partial(form_kernel, slots), out_shape=jax.ShapeDtypeStruct((1,), jnp.int32),
                          in_specs=[smem], out_specs=smem, name="form")(step_counts)


def per_device(lat_count, lon_count, state, winds, diffusivity, sounding_cell, sounding_owner,
               step_counts, channel_list, absorb_table, emit_table, obs_weight, observed):
    width = state.shape[-1]
    operands = (
        step_counts, state.reshape(-1, width), winds.reshape(-1, width), diffusivity,
        jnp.transpose(observed[:, 0], (0, 2, 1, 3)), absorb_table.T, emit_table.T,
        sounding_cell, jnp.transpose(sounding_owner, (0, 2, 1)), channel_list.reshape(-1, LANES),
        obs_weight)
    slots = step_counts.shape[0]
    branches = [partial(whole_call, lat_count, lon_count, n) for n in range(slots, slots * MAXSTEP + 1)]
    return lax.switch(form_of(step_counts, slots)[0], branches, *operands).reshape(state.shape)


def solution(mesh):
    return jax.shard_map(
        partial(per_device, mesh.shape["lat"], mesh.shape["lon"]),
        mesh=mesh,
        in_specs=(
            P(None, None, "lat", "lon"),
            P(None, None, "lat", "lon"),
            P("lat", "lon"),
            P(None, ("lon", "lat")),
            P(None, ("lon", "lat"), None),
            P(),
            P(),
            P(),
            P(),
            P(),
            P(None, ("lon", "lat"), None, None, None),
        ),
        out_specs=P(None, None, "lat", "lon"),
        check_vma=False,
    )
```
